32 devices in a mesh: dp: 4 (over y, x), ctx: 8 (over z, core).
Axes of the slice: x: 2, y: 2, z: 4, core: 2. Of those that a mesh axis runs over, the one named last changes fastest.
Arguments:
- layer_input: bfloat16 [4, 1024, 7168], P(None, 'ctx', 'dp'), may hold values from -6 to 6
- kv_latent: bfloat16 [4, 1024, 512], P('dp', 'ctx'), may hold values from -8 to 8
- key_rope: bfloat16 [4, 1024, 64], P('dp', 'ctx'), may hold values from -6 to 6
- q_latent: bfloat16 [4, 1024, 8, 512], P('dp', 'ctx'), may hold values from -60 to 60
- q_rope: bfloat16 [4, 1024, 8, 64], P('dp', 'ctx'), may hold values from -3 to 3
- saved_output: bfloat16 [4, 1024, 8, 512], P('dp', 'ctx'), may hold values from -4 to 4
- w_uv: bfloat16 [512, 1024], replicated, may hold values from -0.25 to 0.25
- d_out: bfloat16 [4, 1024, 1024], P('dp', 'ctx'), may hold values from -6 to 6
- blocks: int32 [16], replicated, may hold values from 0 to 15, each once
Outputs:
- d_q_latent: bfloat16 [4, 1024, 8, 512], P('dp', 'ctx')
- d_q_rope: bfloat16 [4, 1024, 8, 64], P('dp', 'ctx')
- d_kv_latent: bfloat16 [4, 1024, 512], P('dp', 'ctx')
- d_key_rope: bfloat16 [4, 1024, 64], P('dp', 'ctx')
- grad_w_down: float32 [7168, 576], P(('dp', 'ctx'))
- grad_w_uv: float32 [512, 1024], P(('dp', 'ctx'))
The draws below stay inside these ranges and needn't reach their ends.
Inputs may be any that keep to these rules, and one draw needn't show every extreme that they name: A permutation: blocks[k] is the position block of rows k * 64 to (k + 1) * 64 - 1 of every sequence.
All inputs are finite; a program needn't handle non-finite values.
Results may differ from the reference program's by a relative error of at most 0.028.
Values may be sent and summed in bfloat16 or wider, within the bound.
A program may use at most 128 MiB of HBM per device.

```python
import functools
import math
import jax
import jax.numpy as jnp
from jax import lax

D = 7168
KVL = 512
ROPE = 64
VHEAD = 128
HEADS = 8
TOK_DEV = 128
SEQ = 1024
N_DP = 4
N_CTX = 8


def base_latent(key):
    return jnp.clip(jax.random.normal(jax.random.fold_in(key, 7), (N_DP, SEQ, KVL), jnp.float32), -6.0, 6.0)


def draw_kv_latent(key, part):
    latent = base_latent(key)
    return latent.astype(jnp.bfloat16)


def draw_q_latent(key, part):
    queries = 0.5 * jnp.clip(jax.random.normal(jax.random.fold_in(key, 9), (N_DP, SEQ, HEADS, KVL), jnp.float32), -6.0, 6.0)
    return queries.astype(jnp.bfloat16)


def strengthened(drawn, own_key, source, target, blocks, factor):
    owner, partner = [(jnp.arange(drawn.shape[axis_at]) // (drawn.shape[axis_at] // blocks)).reshape([-1 if axis == axis_at else 1 for axis in range(drawn.ndim)]) for axis_at in (source, target)]
    chosen = jax.random.permutation(own_key, blocks)[partner]
    strong = (owner == chosen) | (owner == (partner + blocks // 2) % blocks)
    return jnp.where(strong, factor * drawn, drawn)


def block_levels(rng, shape, shards, smallest, high):
    factor_of, own = 1.0, jax.random.fold_in(rng, 6)
    for dim, blocks in shards:
        steps = jnp.exp(jax.random.uniform(jax.random.fold_in(own, dim), (blocks,), jnp.float32, smallest / len(shards), high / len(shards)))
        factor_of = factor_of * jnp.repeat(steps, shape[dim] // blocks).reshape([-1 if axis == dim else 1 for axis in range(len(shape))])
    return factor_of


def scatter_about(stream_key, shape, width, limit, split=(), kind=jnp.bfloat16):
    level = block_levels(stream_key, shape, split, -0.22, 0.18) if split else 1.0
    values = jax.random.normal(stream_key, shape, jnp.float32) * width * level
    return jnp.minimum(jnp.maximum(values, -limit), limit).astype(kind)


def bell_draw_with(key, shape, spread, most, split, heavy, kind=jnp.bfloat16):
    drawn = spread * jax.random.normal(key, shape, jnp.float32)
    if split:
        drawn = drawn * block_levels(key, shape, split, -0.22, 0.18)
    return jnp.clip(strengthened(drawn, jax.random.fold_in(key, 3), *heavy), -most, most).astype(kind)


def setup_inputs(seed: int = 0) -> dict:
    splits = jax.random.split(jax.random.key(seed), 10)
    return {
        "layer_input": bell_draw_with(splits[0], (N_DP, SEQ, D), 1.0, 6.0, ((1, 8), (2, 4)), (1, 2, 8, 2.0)),
        "kv_latent": draw_kv_latent(jax.random.fold_in(splits[9], 71), 0),
        "key_rope": scatter_about(splits[2], (N_DP, SEQ, ROPE), 1.0, 6.0, ((0, 4), (1, 8))),
        "q_latent": draw_q_latent(jax.random.fold_in(splits[9], 71), 0),
        "q_rope": scatter_about(splits[4], (N_DP, SEQ, HEADS, ROPE), 0.5, 3.0, ((0, 4), (1, 8))),
        "saved_output": scatter_about(splits[5], (N_DP, SEQ, HEADS, KVL), 0.5, 4.0, ((0, 4), (1, 8))),
        "w_uv": scatter_about(splits[6], (KVL, HEADS * VHEAD), KVL ** -0.5, 0.25),
        "d_out": scatter_about(splits[7], (N_DP, SEQ, HEADS * VHEAD), 1.0, 6.0, ((0, 4), (1, 8))),
        "blocks": jax.random.permutation(splits[8], 2 * N_CTX).astype(jnp.int32),
    }


softmax_scale = 1.0 / math.sqrt(192.0)

def group_grads(carry, group, latent_keys, rope_keys, positions, value_weight):
    term_lat, term_rope, value_total = carry
    query_lat, query_rope, saved_rows, grad_out, query_pos = group
    wide = jnp.float32
    keys_wide = latent_keys.astype(wide)
    rope_wide = rope_keys.astype(wide)
    scores = jnp.einsum('thk,jk->thj', query_lat.astype(wide), keys_wide)
    scores = scores + jnp.einsum('thr,jr->thj', query_rope.astype(wide), rope_wide)
    scores = scores * softmax_scale
    visible = positions[None, None, :] <= query_pos[:, None, None]
    masked = jnp.where(visible, scores, -jnp.inf)
    row_max = lax.optimization_barrier(jnp.max(masked, axis=2, keepdims=True))
    log_total = row_max + jnp.log(lax.optimization_barrier(jnp.sum(jnp.exp(masked - row_max), axis=2, keepdims=True)))
    probs = jnp.exp(masked - log_total)
    probs_low = probs.astype(jnp.bfloat16)
    grad_lat = jnp.einsum('thv,khv->thk', grad_out.astype(wide), value_weight.astype(wide)).astype(jnp.bfloat16)
    delta = lax.optimization_barrier(jnp.sum(grad_lat.astype(wide) * saved_rows.astype(wide), axis=2, keepdims=True))
    grad_prob = jnp.einsum('thk,jk->thj', grad_lat.astype(wide), keys_wide)
    grad_score = (probs * (grad_prob - delta)).astype(jnp.bfloat16)
    score_wide = grad_score.astype(wide)
    dq_lat = (softmax_scale * jnp.einsum('thj,jk->thk', score_wide, keys_wide)).astype(jnp.bfloat16)
    dq_rope = (softmax_scale * jnp.einsum('thj,jr->thr', score_wide, rope_wide)).astype(jnp.bfloat16)
    part_lat = jnp.einsum('thj,thk->jk', probs_low.astype(wide), grad_lat.astype(wide))
    part_lat = part_lat + softmax_scale * jnp.einsum('thj,thk->jk', score_wide, query_lat.astype(wide))
    part_rope = softmax_scale * jnp.einsum('thj,thr->jr', score_wide, query_rope.astype(wide))
    term_lat = term_lat + lax.optimization_barrier(part_lat.astype(jnp.bfloat16)).astype(wide)
    term_rope = term_rope + lax.optimization_barrier(part_rope.astype(jnp.bfloat16)).astype(wide)
    value_total = value_total + jnp.einsum('thk,thv->khv', saved_rows.astype(wide), grad_out.astype(wide))
    return ((term_lat, term_rope, value_total), (dq_lat, dq_rope))

def reference(layer_input, kv_latent, key_rope, q_latent, q_rope, saved_output, w_uv, d_out, blocks):
    half_rows = TOK_DEV // 2
    row_ids = jnp.arange(SEQ, dtype=jnp.int32)
    positions = (blocks[row_ids // half_rows] * half_rows + row_ids % half_rows).astype(jnp.int32)
    value_weight = w_uv.reshape(KVL, HEADS, VHEAD)
    query_pos = positions.reshape(N_CTX, TOK_DEV)
    value_total = jnp.zeros((KVL, HEADS, VHEAD), jnp.float32)
    down_total = jnp.zeros((D, KVL + ROPE), jnp.float32)
    dql_list, dqr_list, dkv_list, dkr_list = ([], [], [], [])
    for seq_index in range(N_DP):
        groups = (q_latent[seq_index].reshape(N_CTX, TOK_DEV, HEADS, KVL), q_rope[seq_index].reshape(N_CTX, TOK_DEV, HEADS, ROPE), saved_output[seq_index].reshape(N_CTX, TOK_DEV, HEADS, KVL), d_out[seq_index].reshape(N_CTX, TOK_DEV, HEADS, VHEAD), query_pos)
        step_fn = functools.partial(group_grads, latent_keys=kv_latent[seq_index], rope_keys=key_rope[seq_index], positions=positions, value_weight=value_weight)
        start = (jnp.zeros((SEQ, KVL), jnp.float32), jnp.zeros((SEQ, ROPE), jnp.float32), value_total)
        (term_lat, term_rope, value_total), (dq_lat, dq_rope) = lax.scan(step_fn, start, groups)
        dkv_low = term_lat.astype(jnp.bfloat16)
        dkr_low = term_rope.astype(jnp.bfloat16)
        joined = jnp.concatenate([dkv_low, dkr_low], axis=1)
        down_total = down_total + jnp.dot(layer_input[seq_index].T, joined, preferred_element_type=jnp.float32)
        dql_list.append(dq_lat.reshape(SEQ, HEADS, KVL))
        dqr_list.append(dq_rope.reshape(SEQ, HEADS, ROPE))
        dkv_list.append(dkv_low)
        dkr_list.append(dkr_low)
    return (jnp.stack(dql_list), jnp.stack(dqr_list), jnp.stack(dkv_list), jnp.stack(dkr_list), down_total, value_total.reshape(KVL, HEADS * VHEAD))
```

```python
import functools
import math

import jax
import jax.numpy as jnp
from jax import lax
from jax.experimental import pallas as pl
from jax.experimental.pallas import tpu as pltpu
from jax.sharding import PartitionSpec as P

softmax_scale = 1.0 / math.sqrt(192.0)
score_scale = softmax_scale / math.log(2.0)
hidden_score = -1e30
wide = jnp.float32
low = jnp.bfloat16
MESH = pl.DeviceIdType.MESH
VMEM_LIMIT = 58 * 1024 * 1024
HYBRID = False


def dot(a, b, ca, cb):
    return lax.dot_general(a, b, (((ca,), (cb,)), ((), ())), preferred_element_type=wide)


def remote(src, dst, send, recv, peer):
    return pltpu.make_async_remote_copy(
        src_ref=src, dst_ref=dst, send_sem=send, recv_sem=recv, device_id=peer, device_id_type=MESH
    )


def pick(z, values):
    values = [int(v) for v in values]
    if all(v == values[0] for v in values):
        return values[0]
    out = values[0]
    for at, v in enumerate(values[1:], 1):
        out = jnp.where(z == at, v, out)
    return out


def flag(z, values):
    values = [bool(v) for v in values]
    if all(values) or not any(values):
        return values[0]
    return pick(z, values) == 1


def when(condition, action):
    if condition is True:
        action()
    elif condition is not False:
        pl.when(condition)(action)


def otherwise(condition, action):
    if condition is False:
        action()
    elif condition is not True:
        pl.when(jnp.logical_not(condition))(action)


class Line:
    def __init__(self, n):
        self.n, self.hybrid = n, HYBRID and n >= 4
        far = lambda z: sorted([d for d in range(n) if d != z], key=lambda d: (-abs(d - z), d))
        self.near = [sorted([d for d in range(n) if d != z], key=lambda d: (abs(d - z), d)) for z in range(n)]
        self.gather = [[d for d in far(z) if not self.ends(z, d)] + [d for d in far(z) if self.ends(z, d)] for z in range(n)]
        self.reduce = []
        for z in range(n):
            order = far(z)
            relayed = [d for d in order if self.consumes(z, d)]
            self.reduce.append([d for d in order if d not in relayed] + relayed + [z])

    def ends(self, z, d):
        return self.hybrid and {z, d} == {0, self.n - 1}

    def consumes(self, z, d):
        return self.hybrid and (z, d) in ((1, self.n - 1), (self.n - 2, 0))

    def column(self, table, at):
        return [row[at] for row in table]


def main_kernel(
    n_dp, n_ctx,
    blocks_ref, lat_hbm, rope_hbm, ql_hbm, qr_hbm, saved_hbm, weight_hbm, out_hbm, layer_hbm,
    dql_ref, dqr_ref, dlat_ref, drope_ref, down_ref, uv_ref,
    lat_all, rope_all, kr2, ql, qrt, qrf, qr2, qr2t, saved, weight, dout, layer, turned,
    spread, grad, delta, posk, expo, slope, tops, sums, factor,
    val_parts, val_landed, val_total, val_term, val_pair, val_sum, val_in,
    own_a, term_a, pair_a, sum_a, in_a, relay_a, acc_a, msg_a, blocks_a,
    own_b, term_b, pair_b, sum_b, in_b, relay_b, acc_b, msg_b, blocks_b,
    own_c, term_c, pair_c, sum_c, in_c, relay_c, acc_c,
    own_d, term_d, pair_d, sum_d, in_d, relay_d, acc_d,
    rope_lo, rope_hi,
    local_sem, key_send, key_recv, fwd_send, fwd_recv, relay_send,
    val_send, val_recv, vp_send, vp_recv, vz_send, vz_recv,
    pair_send, pair_recv, z_send, z_recv, rl_recv, dp_send, dp_recv,
):
    dp, ctx = lax.axis_index("dp"), lax.axis_index("ctx")
    n_z = n_ctx // 2
    z, core = ctx // 2, ctx % 2
    other = 1 - core
    line = Line(n_z)
    partner = (dp, z * 2 + other)
    chip_peer = lambda c: (dp, c * 2 + core)
    dp_peer = lambda k: (lax.rem(dp + k, n_dp), ctx)
    tokens, latent = lat_hbm.shape
    rope_width = rope_hbm.shape[0]
    rows = ql.shape[0]
    heads = rows // tokens
    half = tokens // 2
    chip_rows = 2 * tokens
    values = dout.shape[1]
    part = latent // 2
    pending = []

    def local(at, src, dst):
        copy = pltpu.make_async_copy(src, dst, local_sem.at[at])
        copy.start()
        return copy

    lat_in = local(0, lat_hbm, lat_all.at[ctx])
    rope_in = local(1, rope_hbm, rope_all.at[ctx])
    out_in = local(2, out_hbm, dout)
    qr_in = local(3, qr_hbm, qrt)
    saved_in = local(4, saved_hbm, saved)
    weight_in = local(5, weight_hbm, weight)
    ql_in = local(6, ql_hbm, ql)
    layer_in = local(7, layer_hbm, layer)

    peers = [partner]
    peers += [chip_peer(lax.rem(z + k, n_z)) for k in range(1, n_z)]
    peers += [dp_peer(k) for k in range(1, n_dp)]
    barrier = pltpu.get_barrier_semaphore()
    for peer in peers:
        pl.semaphore_signal(barrier, inc=1, device_id=peer, device_id_type=MESH)
    for j in range(2 * n_ctx):
        posk[j * half : (j + 1) * half, :] = blocks_ref[j] * half + lax.broadcasted_iota(jnp.int32, (half, 1), 0)
    lat_in.wait()
    rope_in.wait()
    pl.semaphore_wait(barrier, len(peers))

    def key_copies(owner, sends, recvs, send_at, recv_at, peer):
        index = owner * 2 + core
        return [
            remote(lat_all.at[index], lat_all.at[index], sends.at[send_at], recvs.at[recv_at], peer),
            remote(
                rope_all.at[index], rope_all.at[index], sends.at[n_z + send_at], recvs.at[n_z + recv_at], peer
            ),
        ]

    def start_all(copies):
        for copy in copies:
            copy.start()

    def send_waits(copies):
        for copy in copies:
            copy.wait_send()

    def key_recv_wait(owner):
        for copy in key_copies(owner, key_send, key_recv, 0, owner, partner):
            copy.wait_recv()

    for at in range(n_z - 1):
        dest = pick(z, line.column(line.gather, at))
        ok = flag(z, [not line.ends(c, line.gather[c][at]) for c in range(n_z)])
        copies = key_copies(z, key_send, key_recv, at, z, chip_peer(dest))
        when(ok, functools.partial(start_all, copies))
        pending.append((ok, copies))
    copies = key_copies(z, fwd_send, fwd_recv, z, z, partner)
    start_all(copies)
    pending.append((True, copies))

    out_in.wait()
    lane = lax.broadcasted_iota(jnp.int32, (heads, values), 1)
    head = lax.broadcasted_iota(jnp.int32, (heads, values), 0)
    keep = (lane // (values // heads) == head)[None]
    group = min(16, tokens)
    for start in range(0, tokens, group):
        piece = dout[start : start + group].astype(wide)
        piece = jnp.broadcast_to(piece[:, None, :], (group, heads, values))
        piece = jnp.where(keep, piece, 0.0).reshape(group * heads, values)
        spread[start * heads : (start + group) * heads, :] = piece.astype(low)

    qr_in.wait()
    two = 2 * rope_width
    lower = lax.broadcasted_iota(jnp.int32, (tokens, two), 1) < rope_width
    for at in range(heads // 2):
        piece = qrt[2 * at : 2 * at + 2].reshape(two, tokens).astype(wide).T
        qrf[pl.ds(2 * at, tokens, stride=heads), :] = jnp.where(lower, piece, 0.0)
        qrf[pl.ds(2 * at + 1, tokens, stride=heads), :] = jnp.where(lower, 0.0, piece)
    qr2[...] = qrf[...].astype(low)
    qr2t[...] = qrf[...].T.astype(low)

    saved_in.wait()
    weight_in.wait()
    tile = min(256, rows)
    for start in range(0, rows, tile):
        piece = dot(spread[start : start + tile], weight[...], 1, 1).astype(low)
        grad[start : start + tile, :] = piece
        prod = piece.astype(wide) * saved[start : start + tile].astype(wide)
        total = prod[:, :128]
        for at in range(128, prod.shape[1], 128):
            total = total + prod[:, at : at + 128]
        delta[:, start : start + tile] = jnp.sum(total.T, axis=0, keepdims=True)
    ql_in.wait()

    low_block, high_block = blocks_ref[2 * ctx], blocks_ref[2 * ctx + 1]

    def pass_on(owner):
        copies = key_copies(owner, fwd_send, fwd_recv, owner, owner, partner)
        start_all(copies)
        pending.append((True, copies))

    def chunk(owner):
        for copy in key_copies(owner, fwd_send, fwd_recv, 0, owner, partner):
            copy.wait_recv()
        keys = pl.ds(pl.multiple_of(owner * chip_rows, chip_rows), chip_rows)
        for at in range(2):
            piece = rope_all[owner * 2 + at].astype(wide)
            kr2[pl.ds(pl.multiple_of((owner * 2 + at) * tokens, tokens), tokens), :] = (
                jnp.concatenate([piece, piece], axis=0).T.astype(low)
            )

        def score_tile(i, carry):
            if isinstance(i, int):
                span = pl.ds(i * tile, tile)
            else:
                span = pl.ds(pl.multiple_of(i * tile, tile), tile)
            key_lat = lat_all[pl.ds(owner * 2, 2)].reshape(chip_rows, latent)
            scores = dot(key_lat, ql[span, :], 1, 1) + dot(kr2[keys, :], qr2[span, :], 1, 1)
            token = (i * tile + lax.broadcasted_iota(jnp.int32, (1, tile), 1)) // heads
            posq = jnp.where(token < half, low_block * half + token, high_block * half + token - half)
            scores = jnp.where(posk[keys, :] <= posq, scores * score_scale, hidden_score)
            top = jnp.max(scores, axis=0, keepdims=True)
            piece = jnp.exp2(scores - top)
            tops[owner, :, span] = top
            sums[owner, :, span] = jnp.sum(piece, axis=0, keepdims=True)
            expo[keys, span] = piece.astype(low)
            grad_prob = dot(key_lat, grad[span, :], 1, 1)
            slope[keys, span] = (piece * (grad_prob - delta[:, span])).astype(low)
            return carry

        if n_z <= 4:
            for i in range(rows // tile):
                score_tile(i, 0)
        else:
            lax.fori_loop(0, rows // tile, score_tile, 0)

    chunk(z)

    share = val_parts.shape[1]
    value = dot(saved[...], spread[...], 0, 0).astype(low)
    for d in range(n_dp):
        val_parts[d] = value[d * share : (d + 1) * share]
    value_copies = []
    for k in range(1, n_dp):
        copy = remote(
            val_parts.at[lax.rem(dp + k, n_dp)], val_landed.at[k], val_send.at[k], val_recv.at[k], dp_peer(k)
        )
        copy.start()
        value_copies.append(copy)
    pending.append((True, value_copies))

    height = down_ref.shape[0]
    padded = turned.shape[1]
    batch = layer.shape[0]

    def turn():
        layer_in.wait()
        for d in range(batch):
            piece = layer[d].T
            for c in range(n_ctx):
                rows_c = piece[c * height : (c + 1) * height]
                if padded > height:
                    rows_c = jnp.concatenate(
                        [rows_c.astype(wide), jnp.zeros((padded - height, tokens), wide)], axis=0
                    ).astype(low)
                turned[c, :, d * tokens : (d + 1) * tokens] = rows_c

    for at in range(n_z - 1):
        owner = pick(z, line.column(line.near, at))
        key_recv_wait(owner)
        pass_on(owner)
        relay_ok = flag(z, [line.hybrid and (c, line.near[c][at]) in ((1, n_z - 1), (n_z - 2, 0)) for c in range(n_z)])
        if relay_ok is not False:
            end = jnp.where(z == 1, 0, n_z - 1)
            index = owner * 2 + core
            copies = [
                remote(lat_all.at[index], lat_all.at[index], relay_send.at[0], key_recv.at[owner], chip_peer(end)),
                remote(
                    rope_all.at[index], rope_all.at[index], relay_send.at[1], key_recv.at[n_z + owner], chip_peer(end)
                ),
            ]
            when(relay_ok, functools.partial(start_all, copies))
            pending.append((relay_ok, copies))
        if at == n_z - 2:
            turn()
        chunk(owner)

    top = tops[0]
    for c in range(1, n_z):
        top = jnp.maximum(top, tops[c])
    total = jnp.zeros_like(top)
    for c in range(n_z):
        weight_c = jnp.exp2(tops[c] - top)
        factor[c] = weight_c
        total = total + sums[c] * weight_c
    inverse = 1.0 / total
    for c in range(n_z):
        factor[c] = factor[c] * inverse

    def pair_copy(s, at, term, landing):
        return remote(term.at[at], landing.at[at], pair_send.at[s * n_z + at], pair_recv.at[s * n_z + at], partner)

    def relay_copy(s, at, sums_out, relay_in):
        neighbour = jnp.where(z == 0, 1, n_z - 2)
        return remote(sums_out.at[at], relay_in, z_send.at[s * n_z + at], rl_recv.at[s], chip_peer(neighbour))

    def reduce_set(s, compute, own, term, landing, sums_out, z_in, relay_in, acc):
        def finish(at):
            pair_copy(s, at, term, landing).wait_recv()
            added = own[at % 2] + landing[at].astype(wide)
            if at == n_z - 1:
                acc[...] = added
                return
            consumer = flag(z, [line.consumes(c, line.reduce[c][at]) for c in range(n_z)])

            def with_relay():
                relay_copy(s, at, sums_out, relay_in).wait_recv()
                sums_out[at] = (added + relay_in[...].astype(wide)).astype(low)

            def without():
                sums_out[at] = added.astype(low)

            when(consumer, with_relay)
            otherwise(consumer, without)
            dest = pick(z, line.column(line.reduce, at))
            origin = flag(z, [line.ends(c, line.reduce[c][at]) for c in range(n_z)])
            straight = remote(
                sums_out.at[at], z_in.at[z], z_send.at[s * n_z + at], z_recv.at[s * n_z + z], chip_peer(dest)
            )
            if origin is not False:
                when(origin, lambda: relay_copy(s, at, sums_out, relay_in).start())
            otherwise(origin, lambda: straight.start())
            pending.append((True, [straight]))

        for at in range(n_z):
            dest = pick(z, line.column(line.reduce, at))
            compute(at, dest)
            copy = pair_copy(s, at, term, landing)
            copy.start()
            pending.append((True, [copy]))
            if at > 0:
                finish(at - 1)
        finish(n_z - 1)

    def collect(s, sums_out, z_in, acc):
        for at in range(n_z - 1):
            source = pick(z, line.column(line.near, at))
            ok = flag(z, [not line.ends(c, line.near[c][at]) for c in range(n_z)])

            def add():
                remote(
                    sums_out.at[0], z_in.at[source], z_send.at[s * n_z], z_recv.at[s * n_z + source], partner
                ).wait_recv()
                acc[...] += z_in[source].astype(wide)

            when(ok, add)

    def keys_of(c):
        return pl.ds(pl.multiple_of(c * chip_rows, chip_rows), chip_rows)

    def term_first(at, dest):
        keys = keys_of(dest)
        scale = factor[dest]
        expo[keys, :] = (expo[keys, :].astype(wide) * scale).astype(low)
        slope[keys, :] = (slope[keys, :].astype(wide) * (scale * softmax_scale)).astype(low)
        value = dot(expo[keys, :], grad[:, :part], 1, 0) + dot(slope[keys, :], ql[:, :part], 1, 0)
        stage_a[0] = value[:tokens]
        stage_a[1] = value[tokens:]
        own_a[at % 2] = stage_a[core]
        term_a[at] = stage_a[other].astype(low)

    def term_second(at, dest):
        keys = keys_of(dest)
        value = dot(expo[keys, :], grad[:, part:], 1, 0) + dot(slope[keys, :], ql[:, part:], 1, 0)
        rope = dot(qr2t[...], slope[keys, :], 1, 1)
        rope = rope[:rope_width] + rope[rope_width:]
        quarter = rope_width // 2
        for c in range(2):
            stage_b[c, :tokens, :] = value[c * tokens : (c + 1) * tokens]
            mine = rope[:, c * tokens : (c + 1) * tokens]
            stage_b[c, tokens:, :] = jnp.concatenate([mine[:quarter], mine[quarter:]], axis=1)
        own_b[at % 2] = stage_b[core]
        term_b[at] = stage_b[other].astype(low)

    stage_a, stage_b = own_a.at[pl.ds(2, 2)], own_b.at[pl.ds(2, 2)]
    reduce_set(0, term_first, own_a, term_a, pair_a, sum_a, in_a, relay_a, acc_a)
    reduce_set(1, term_second, own_b, term_b, pair_b, sum_b, in_b, relay_b, acc_b)

    total = val_parts[dp].astype(wide)
    for k in range(1, n_dp):
        value_copies[k - 1].wait_recv()
        total = total + val_landed[k].astype(wide)
    piece = val_total.shape[1]
    for c in range(n_ctx):
        val_total[c] = total[c * piece : (c + 1) * piece]
    value_pairs = []
    for k in range(n_z):
        dest = lax.rem(z + k, n_z)
        val_term[k] = val_total[dest * 2 + other].astype(low)
        copy = remote(val_term.at[k], val_pair.at[k], vp_send.at[k], vp_recv.at[k], partner)
        copy.start()
        value_pairs.append(copy)
    pending.append((True, value_pairs))

    def query_tile(i, carry):
        if isinstance(i, int):
            span = pl.ds(i * tile, tile)
        else:
            span = pl.ds(pl.multiple_of(i * tile, tile), tile)
        piece = slope[:, span]
        all_lat = lat_all[...].reshape(n_ctx * tokens, latent)
        dql_ref[span, :] = dot(piece, all_lat, 0, 0).astype(low)
        qrf[span, :] = dot(piece, kr2[...], 0, 0)
        return carry

    lax.fori_loop(0, rows // tile, query_tile, 0)
    for at in range(heads // 2):
        even = qrf[pl.ds(2 * at, tokens, stride=heads), :]
        odd = qrf[pl.ds(2 * at + 1, tokens, stride=heads), :]
        piece = jnp.where(lower, even, odd).T.astype(low)
        dqr_ref[2 * at] = piece[:rope_width]
        dqr_ref[2 * at + 1] = piece[rope_width:]

    value_sends = []
    for k in list(range(1, n_z)) + [0]:
        value_pairs[k].wait_recv()
        dest = lax.rem(z + k, n_z)
        added = val_total[dest * 2 + core] + val_pair[k].astype(wide)
        if k == 0:
            uv_ref[...] = added
        else:
            val_sum[k] = added.astype(low)
            copy = remote(val_sum.at[k], val_in.at[k], vz_send.at[k], vz_recv.at[k], chip_peer(dest))
            copy.start()
            value_sends.append(copy)
    pending.append((True, value_sends))

    def spread_dp(s, acc, msg, landing):
        msg[...] = acc[...].astype(low)
        landing[dp] = msg[...]
        copies = []
        for k in range(1, n_dp):
            copy = remote(
                msg, landing.at[dp], dp_send.at[s * n_dp + k], dp_recv.at[s * n_dp + k], dp_peer(k)
            )
            copy.start()
            copies.append(copy)
        pending.append((True, copies))
        return copies

    collect(0, sum_a, in_a, acc_a)
    first = spread_dp(0, acc_a, msg_a, blocks_a)
    dlat_ref[:, :part] = msg_a[...]
    collect(1, sum_b, in_b, acc_b)
    second = spread_dp(1, acc_b, msg_b, blocks_b)
    dlat_ref[:, part:] = msg_b[:tokens, :]
    quarter = rope_width // 2
    drope_ref[:quarter, :] = msg_b[tokens:, :tokens]
    drope_ref[quarter:, :] = msg_b[tokens:, tokens:]

    for copy in first:
        copy.wait_recv()

    def down_first(at, dest):
        every = blocks_a[...].reshape(batch * tokens, part)
        term_c[at] = dot(turned[dest * 2 + other], every, 1, 0).astype(low)
        own_c[at % 2] = dot(turned[dest * 2 + core], every, 1, 0)

    reduce_set(2, down_first, own_c, term_c, pair_c, sum_c, in_c, relay_c, acc_c)

    for copy in second:
        copy.wait_recv()
    packed = height % 32 == 0
    for b in range(batch):
        piece = blocks_b[b, tokens:, :]
        cols = slice(b * tokens, (b + 1) * tokens)
        for at in range(2):
            rope_lo[at * quarter : (at + 1) * quarter, cols] = piece[:, at * tokens : (at + 1) * tokens]
            rope_hi[rope_width + at * quarter : rope_width + (at + 1) * quarter, cols] = piece[
                :, at * tokens : (at + 1) * tokens
            ]
    rope_lo[rope_width:, :] = jnp.zeros((rope_width, batch * tokens), low)
    rope_hi[:rope_width, :] = jnp.zeros((rope_width, batch * tokens), low)

    def down_piece(index):
        every = blocks_b[:, :tokens, :].reshape(batch * tokens, part)
        lat = dot(turned[index], every, 1, 0)
        if packed:
            rope = dot(turned[index, : height // 2], rope_lo[...], 1, 1)
            rope = rope + dot(turned[index, height // 2 :], rope_hi[...], 1, 1)
            rope = jnp.concatenate([rope[: height // 4], rope[height // 4 :]], axis=1)
        else:
            rope = dot(turned[index], rope_lo[...], 1, 1)
            rope = jnp.concatenate([rope, jnp.zeros((padded, part - two), wide)], axis=1)
        return lat, rope

    def down_second(at, dest):
        lat, rope = down_piece(dest * 2 + other)
        term_d[at, :padded, :] = lat.astype(low)
        term_d[at, padded:, :] = rope.astype(low)
        lat, rope = down_piece(dest * 2 + core)
        own_d[at % 2, :padded, :] = lat
        own_d[at % 2, padded:, :] = rope

    reduce_set(3, down_second, own_d, term_d, pair_d, sum_d, in_d, relay_d, acc_d)
    for k in range(1, n_z):
        value_sends[k - 1].wait_recv()
        uv_ref[...] += val_in[k].astype(wide)
    collect(2, sum_c, in_c, acc_c)
    down_ref[:, :part] = acc_c[:height, :]
    collect(3, sum_d, in_d, acc_d)
    down_ref[:, part:latent] = acc_d[:height, :]
    if packed:
        rope = acc_d[padded:, :]
        rope = jnp.concatenate([rope[:, :two], rope[:, two:]], axis=0)
        down_ref[: height // 2, latent:] = rope[:, :rope_width]
        down_ref[height // 2 :, latent:] = rope[:, rope_width:]
    else:
        down_ref[:, latent:] = acc_d[padded : padded + height, :rope_width]

    for ok, copies in pending:
        when(ok, functools.partial(send_waits, copies))


def store_kernel(n, *refs):
    sem = refs[2 * n]
    copies = [pltpu.make_async_copy(refs[at], refs[n + at], sem.at[at]) for at in range(n)]
    for copy in copies:
        copy.start()
    for copy in copies:
        copy.wait()


def body(n_dp, n_ctx, layer_input, kv_latent, key_rope, q_latent, q_rope, saved_output, w_uv, d_out, blocks):
    tokens = kv_latent.shape[1]
    heads, latent = q_latent.shape[2], q_latent.shape[3]
    rope_width = key_rope.shape[2]
    rows = tokens * heads
    seq_rows = tokens * n_ctx
    n_z = n_ctx // 2
    values = w_uv.shape[1]
    batch, _, width = layer_input.shape
    height = width // n_ctx
    padded = -(-height // 16) * 16
    extra = height // 4 if height % 32 == 0 else padded
    share = latent // (n_dp * n_ctx)
    part = latent // 2
    two = 2 * rope_width
    vmem = pl.BlockSpec(memory_space=pltpu.VMEM)
    hbm = pl.BlockSpec(memory_space=pltpu.HBM)
    dma = lambda n: pltpu.SemaphoreType.DMA((n,))

    def stage(count, fill, landed):
        half = lambda *dims: pltpu.VMEM((*dims, fill, part), low)
        out = [
            pltpu.VMEM((count, fill, part), wide), half(n_z), half(n_z), half(n_z), half(n_z), half(),
            pltpu.VMEM((fill, part), wide),
        ]
        return out + ([half(), half(batch)] if landed else [])

    outs = (
        ((rows, latent), low),
        ((heads, rope_width, tokens), low),
        ((tokens, latent), low),
        ((rope_width, tokens), low),
        ((height, latent + rope_width), wide),
        ((share, values), wide),
    )
    found = pl.pallas_call(
        functools.partial(main_kernel, n_dp, n_ctx),
        out_shape=tuple(pltpu.VMEM(shape, kind) for shape, kind in outs),
        in_specs=[pl.BlockSpec(memory_space=pltpu.SMEM)] + [hbm] * 8,
        out_specs=(vmem,) * 6,
        scratch_shapes=[
            pltpu.VMEM((n_ctx, tokens, latent), low),
            pltpu.VMEM((n_ctx, rope_width, tokens), low),
            pltpu.VMEM((seq_rows, two), low),
            pltpu.VMEM((rows, latent), low),
            pltpu.VMEM((heads, rope_width, tokens), low),
            pltpu.VMEM((rows, two), wide),
            pltpu.VMEM((rows, two), low),
            pltpu.VMEM((two, rows), low),
            pltpu.VMEM((rows, latent), low),
            pltpu.VMEM((latent, values), low),
            pltpu.VMEM((tokens, values), low),
            pltpu.VMEM(layer_input.shape, low),
            pltpu.VMEM((n_ctx, padded, batch * tokens), low),
            pltpu.VMEM((rows, values), low),
            pltpu.VMEM((rows, latent), low),
            pltpu.VMEM((1, rows), wide),
            pltpu.VMEM((seq_rows, 1), jnp.int32),
            pltpu.VMEM((seq_rows, rows), low),
            pltpu.VMEM((seq_rows, rows), low),
            pltpu.VMEM((n_z, 1, rows), wide),
            pltpu.VMEM((n_z, 1, rows), wide),
            pltpu.VMEM((n_z, 1, rows), wide),
            pltpu.VMEM((n_dp, latent // n_dp, values), low),
            pltpu.VMEM((n_dp, latent // n_dp, values), low),
            pltpu.VMEM((n_ctx, share, values), wide),
            pltpu.VMEM((n_z, share, values), low),
            pltpu.VMEM((n_z, share, values), low),
            pltpu.VMEM((n_z, share, values), low),
            pltpu.VMEM((n_z, share, values), low),
            *stage(4, tokens, True),
            *stage(4, tokens + rope_width // 2, True),
            *stage(2, padded, False),
            *stage(2, padded + extra, False),
            pltpu.VMEM((two, batch * tokens), low),
            pltpu.VMEM((two, batch * tokens), low),
            dma(8), dma(2 * n_z), dma(2 * n_z), dma(2 * n_z), dma(2 * n_z), dma(2),
            dma(n_dp), dma(n_dp), dma(n_z), dma(n_z), dma(n_z), dma(n_z),
            dma(4 * n_z), dma(4 * n_z), dma(4 * n_z), dma(4 * n_z), dma(4), dma(2 * n_dp), dma(2 * n_dp),
        ],
        compiler_params=pltpu.CompilerParams(
            collective_id=0, has_side_effects=True, vmem_limit_bytes=VMEM_LIMIT
        ),
        name="main",
    )(
        blocks, kv_latent[0], key_rope[0].T,
        q_latent[0].reshape(rows, latent), jnp.transpose(q_rope[0], (1, 2, 0)),
        saved_output[0].reshape(rows, latent), w_uv, d_out[0], layer_input,
    )
    d_lat, d_rope, k_lat, k_rope, grad_down, grad_uv = pl.pallas_call(
        functools.partial(store_kernel, len(outs)),
        out_shape=tuple(jax.ShapeDtypeStruct(shape, kind) for shape, kind in outs),
        in_specs=[vmem] * len(outs),
        out_specs=(hbm,) * len(outs),
        scratch_shapes=[dma(len(outs))],
        compiler_params=pltpu.CompilerParams(vmem_limit_bytes=4 * 1024 * 1024),
        name="store",
    )(*found)
    return (
        d_lat.reshape(1, tokens, heads, latent),
        jnp.transpose(d_rope, (2, 0, 1))[None],
        k_lat[None],
        k_rope.T[None],
        grad_down,
        grad_uv,
    )


def solution(mesh):
    n_dp, n_ctx = mesh.shape["dp"], mesh.shape["ctx"]
    in_specs = (
        P(None, "ctx", "dp"),
        P("dp", "ctx", None),
        P("dp", "ctx", None),
        P("dp", "ctx", None, None),
        P("dp", "ctx", None, None),
        P("dp", "ctx", None, None),
        P(),
        P("dp", "ctx", None),
        P(),
    )
    out_specs = (
        P("dp", "ctx", None, None),
        P("dp", "ctx", None, None),
        P("dp", "ctx", None),
        P("dp", "ctx", None),
        P(("dp", "ctx"), None),
        P(("dp", "ctx"), None),
    )
    return jax.shard_map(
        functools.partial(body, n_dp, n_ctx),
        mesh=mesh, in_specs=in_specs, out_specs=out_specs, check_vma=False,
    )
```

```python
import functools
import math

import jax
import jax.numpy as jnp
from jax import lax
from jax.experimental import pallas as pl
from jax.experimental.pallas import tpu as pltpu
from jax.sharding import PartitionSpec as P

softmax_scale = 1.0 / math.sqrt(192.0)
score_scale = softmax_scale / math.log(2.0)
hidden_score = -1e30
wide = jnp.float32
low = jnp.bfloat16
MESH = pl.DeviceIdType.MESH
VMEM_LIMIT = 58 * 1024 * 1024
HYBRID = True


def dot(a, b, ca, cb):
    return lax.dot_general(a, b, (((ca,), (cb,)), ((), ())), preferred_element_type=wide)


def remote(src, dst, send, recv, peer):
    return pltpu.make_async_remote_copy(
        src_ref=src, dst_ref=dst, send_sem=send, recv_sem=recv, device_id=peer, device_id_type=MESH
    )


def pick(z, values):
    values = [int(v) for v in values]
    if all(v == values[0] for v in values):
        return values[0]
    out = values[0]
    for at, v in enumerate(values[1:], 1):
        out = jnp.where(z == at, v, out)
    return out


def flag(z, values):
    values = [bool(v) for v in values]
    if all(values) or not any(values):
        return values[0]
    return pick(z, values) == 1


def when(condition, action):
    if condition is True:
        action()
    elif condition is not False:
        pl.when(condition)(action)


def otherwise(condition, action):
    if condition is False:
        action()
    elif condition is not True:
        pl.when(jnp.logical_not(condition))(action)


class Line:
    def __init__(self, n):
        self.n, self.hybrid = n, HYBRID and n >= 4
        far = lambda z: sorted([d for d in range(n) if d != z], key=lambda d: (-abs(d - z), d))
        self.near = [sorted([d for d in range(n) if d != z], key=lambda d: (abs(d - z), d)) for z in range(n)]
        first = lambda z: [d for d in self.near[z] if self.forwards(z, d)]
        self.arrive = [first(z) + [d for d in self.near[z] if d not in first(z)] for z in range(n)]
        self.gather = [[d for d in far(z) if not self.ends(z, d)] + [d for d in far(z) if self.ends(z, d)] for z in range(n)]
        self.reduce = []
        for z in range(n):
            order = far(z)
            relayed = [d for d in order if self.consumes(z, d)]
            self.reduce.append([d for d in order if d not in relayed] + relayed + [z])

    def ends(self, z, d):
        return self.hybrid and {z, d} == {0, self.n - 1}

    def consumes(self, z, d):
        return self.hybrid and (z, d) in ((1, self.n - 1), (self.n - 2, 0))

    def forwards(self, z, owner):
        return self.hybrid and (z, owner) in ((1, self.n - 1), (self.n - 2, 0))

    def column(self, table, at):
        return [row[at] for row in table]


def main_kernel(
    n_dp, n_ctx,
    blocks_ref, lat_hbm, rope_hbm, ql_hbm, qr_hbm, saved_hbm, weight_hbm, out_hbm, layer_hbm,
    dql_ref, dqr_ref, dlat_ref, drope_ref, down_ref, uv_ref,
    lat_all, rope_all, kr2, ql, qrt, qrf, qr2, qr2t, saved, weight, dout, layer, turned,
    spread, grad, delta, posk, expo, slope, tops, sums, factor,
    val_parts, val_landed, val_total, val_term, val_pair, val_sum, val_in,
    key_stage, own_k, term_k, pair_k, sum_k, in_k, relay_k, acc_k, message, landed,
    own_d, term_d, pair_d, sum_d, in_d, relay_d, acc_d,
    rope_lo, rope_hi,
    local_sem, key_send, key_recv, fwd_send, fwd_recv, relay_send,
    val_send, val_recv, vp_send, vp_recv, vz_send, vz_recv,
    kp_send, kp_recv, kz_send, kz_recv, kr_recv, gp_send, gp_recv, gz_send, gz_recv, gr_recv, dp_send, dp_recv,
):
    dp, ctx = lax.axis_index("dp"), lax.axis_index("ctx")
    n_z = n_ctx // 2
    z, core = ctx // 2, ctx % 2
    other = 1 - core
    line = Line(n_z)
    partner = (dp, z * 2 + other)
    chip_peer = lambda c: (dp, c * 2 + core)
    dp_peer = lambda k: (lax.rem(dp + k, n_dp), ctx)
    tokens, latent = lat_hbm.shape
    rope_width = rope_hbm.shape[0]
    rows = ql.shape[0]
    heads = rows // tokens
    half = tokens // 2
    chip_rows = 2 * tokens
    values = dout.shape[1]
    pieces = 4
    lanes = latent // pieces
    pending = []

    def local(at, src, dst):
        copy = pltpu.make_async_copy(src, dst, local_sem.at[at])
        copy.start()
        return copy

    lat_in = local(0, lat_hbm, lat_all.at[ctx])
    rope_in = local(1, rope_hbm, rope_all.at[ctx])
    out_in = local(2, out_hbm, dout)
    qr_in = local(3, qr_hbm, qrt)
    saved_in = local(4, saved_hbm, saved)
    weight_in = local(5, weight_hbm, weight)
    ql_in = local(6, ql_hbm, ql)
    layer_in = local(7, layer_hbm, layer)

    peers = [partner]
    peers += [chip_peer(lax.rem(z + k, n_z)) for k in range(1, n_z)]
    peers += [dp_peer(k) for k in range(1, n_dp)]
    barrier = pltpu.get_barrier_semaphore()
    for peer in peers:
        pl.semaphore_signal(barrier, inc=1, device_id=peer, device_id_type=MESH)
    for j in range(2 * n_ctx):
        posk[j * half : (j + 1) * half, :] = blocks_ref[j] * half + lax.broadcasted_iota(jnp.int32, (half, 1), 0)
    lat_in.wait()
    rope_in.wait()
    pl.semaphore_wait(barrier, len(peers))

    def key_copies(owner, sends, recvs, send_at, recv_at, peer):
        index = owner * 2 + core
        refs = [lat_all.at[index, pl.ds(0, half)], lat_all.at[index, pl.ds(half, half)], rope_all.at[index]]
        return [
            remote(ref, ref, sends.at[n * n_z + send_at], recvs.at[n * n_z + recv_at], peer)
            for n, ref in enumerate(refs)
        ]

    def start_all(copies):
        for copy in copies:
            copy.start()

    def send_waits(copies):
        for copy in copies:
            copy.wait_send()

    for at in range(n_z - 1):
        dest = pick(z, line.column(line.gather, at))
        ok = flag(z, [not line.ends(c, line.gather[c][at]) for c in range(n_z)])
        copies = key_copies(z, key_send, key_recv, at, z, chip_peer(dest))
        when(ok, functools.partial(start_all, copies))
        pending.append((ok, copies))
    copies = key_copies(z, fwd_send, fwd_recv, z, z, partner)
    start_all(copies)
    pending.append((True, copies))

    out_in.wait()
    lane = lax.broadcasted_iota(jnp.int32, (heads, values), 1)
    head = lax.broadcasted_iota(jnp.int32, (heads, values), 0)
    keep = (lane // (values // heads) == head)[None]
    group = min(16, tokens)
    for start in range(0, tokens, group):
        piece = dout[start : start + group].astype(wide)
        piece = jnp.broadcast_to(piece[:, None, :], (group, heads, values))
        piece = jnp.where(keep, piece, 0.0).reshape(group * heads, values)
        spread[start * heads : (start + group) * heads, :] = piece.astype(low)

    qr_in.wait()
    two = 2 * rope_width
    lower = lax.broadcasted_iota(jnp.int32, (tokens, two), 1) < rope_width
    for at in range(heads // 2):
        piece = qrt[2 * at : 2 * at + 2].reshape(two, tokens).astype(wide).T
        qrf[pl.ds(2 * at, tokens, stride=heads), :] = jnp.where(lower, piece, 0.0)
        qrf[pl.ds(2 * at + 1, tokens, stride=heads), :] = jnp.where(lower, 0.0, piece)
    qr2[...] = qrf[...].astype(low)
    qr2t[...] = qrf[...].T.astype(low)

    saved_in.wait()
    share = val_parts.shape[1]
    value = dot(saved[...], spread[...], 0, 0).astype(low)
    for d in range(n_dp):
        val_parts[d] = value[d * share : (d + 1) * share]
    value_copies = []
    for k in range(1, n_dp):
        copy = remote(
            val_parts.at[lax.rem(dp + k, n_dp)], val_landed.at[k], val_send.at[k], val_recv.at[k], dp_peer(k)
        )
        copy.start()
        value_copies.append(copy)
    pending.append((True, value_copies))

    weight_in.wait()
    tile = min(256, rows)
    for start in range(0, rows, tile):
        piece = dot(spread[start : start + tile], weight[...], 1, 1).astype(low)
        grad[start : start + tile, :] = piece
        prod = piece.astype(wide) * saved[start : start + tile].astype(wide)
        total = prod[:, :128]
        for at in range(128, prod.shape[1], 128):
            total = total + prod[:, at : at + 128]
        delta[:, start : start + tile] = jnp.sum(total.T, axis=0, keepdims=True)
    ql_in.wait()

    low_block, high_block = blocks_ref[2 * ctx], blocks_ref[2 * ctx + 1]

    def pass_on(owner):
        copies = key_copies(owner, fwd_send, fwd_recv, owner, owner, partner)
        start_all(copies)
        pending.append((True, copies))

    def chunk(owner):
        for copy in key_copies(owner, fwd_send, fwd_recv, 0, owner, partner):
            copy.wait_recv()
        keys = pl.ds(pl.multiple_of(owner * chip_rows, chip_rows), chip_rows)
        for at in range(2):
            piece = rope_all[owner * 2 + at].astype(wide)
            kr2[pl.ds(pl.multiple_of((owner * 2 + at) * tokens, tokens), tokens), :] = (
                jnp.concatenate([piece, piece], axis=0).T.astype(low)
            )

        def score_tile(i, carry):
            if isinstance(i, int):
                span = pl.ds(i * tile, tile)
            else:
                span = pl.ds(pl.multiple_of(i * tile, tile), tile)
            key_lat = lat_all[pl.ds(owner * 2, 2)].reshape(chip_rows, latent)
            scores = dot(key_lat, ql[span, :], 1, 1) + dot(kr2[keys, :], qr2[span, :], 1, 1)
            token = (i * tile + lax.broadcasted_iota(jnp.int32, (1, tile), 1)) // heads
            posq = jnp.where(token < half, low_block * half + token, high_block * half + token - half)
            scores = jnp.where(posk[keys, :] <= posq, scores * score_scale, hidden_score)
            top = jnp.max(scores, axis=0, keepdims=True)
            piece = jnp.exp2(scores - top)
            tops[owner, :, span] = top
            sums[owner, :, span] = jnp.sum(piece, axis=0, keepdims=True)
            expo[keys, span] = piece.astype(low)
            grad_prob = dot(key_lat, grad[span, :], 1, 1)
            slope[keys, span] = (piece * (grad_prob - delta[:, span])).astype(low)
            return carry

        if n_z <= 4:
            for i in range(rows // tile):
                score_tile(i, 0)
        else:
            lax.fori_loop(0, rows // tile, score_tile, 0)

    chunk(z)

    height = down_ref.shape[0]
    padded = turned.shape[1]
    batch = layer.shape[0]

    def turn():
        layer_in.wait()
        for d in range(batch):
            piece = layer[d].T
            for c in range(n_ctx):
                rows_c = piece[c * height : (c + 1) * height]
                if padded > height:
                    rows_c = jnp.concatenate(
                        [rows_c.astype(wide), jnp.zeros((padded - height, tokens), wide)], axis=0
                    ).astype(low)
                turned[c, :, d * tokens : (d + 1) * tokens] = rows_c

    value_pairs, value_sends = [], []

    def pair_values():
        total = val_parts[dp].astype(wide)
        for k in range(1, n_dp):
            value_copies[k - 1].wait_recv()
            total = total + val_landed[k].astype(wide)
        piece = val_total.shape[1]
        for c in range(n_ctx):
            val_total[c] = total[c * piece : (c + 1) * piece]
        for k in range(n_z):
            dest = lax.rem(z + k, n_z)
            val_term[k] = val_total[dest * 2 + other].astype(low)
            copy = remote(val_term.at[k], val_pair.at[k], vp_send.at[k], vp_recv.at[k], partner)
            copy.start()
            value_pairs.append(copy)
        pending.append((True, value_pairs))

    def start_values():
        for k in list(range(1, n_z)) + [0]:
            value_pairs[k].wait_recv()
            dest = lax.rem(z + k, n_z)
            added = val_total[dest * 2 + core] + val_pair[k].astype(wide)
            if k == 0:
                uv_ref[...] = added
            else:
                val_sum[k] = added.astype(low)
                copy = remote(val_sum.at[k], val_in.at[k], vz_send.at[k], vz_recv.at[k], chip_peer(dest))
                copy.start()
                value_sends.append(copy)
        pending.append((True, value_sends))

    for at in range(n_z - 1):
        owner = pick(z, line.column(line.arrive, at))
        relay_ok = flag(z, [line.forwards(c, line.arrive[c][at]) for c in range(n_z)])
        copies = []
        if relay_ok is not False:
            end = jnp.where(z == 1, 0, n_z - 1)
            copies = key_copies(owner, relay_send, key_recv, 0, owner, chip_peer(end))
            pending.append((relay_ok, copies))
        for n, copy in enumerate(key_copies(owner, key_send, key_recv, 0, owner, partner)):
            copy.wait_recv()
            if copies:
                when(relay_ok, copies[n].start)
        pass_on(owner)
        chunk(owner)
        if at == max(n_z - 3, 0):
            turn()

    top = tops[0]
    for c in range(1, n_z):
        top = jnp.maximum(top, tops[c])
    total = jnp.zeros_like(top)
    for c in range(n_z):
        weight_c = jnp.exp2(tops[c] - top)
        factor[c] = weight_c
        total = total + sums[c] * weight_c
    inverse = 1.0 / total
    for c in range(n_z):
        factor[c] = factor[c] * inverse

    lag, slots = 2, 4
    neighbour = jnp.where(z == 0, 1, n_z - 2)

    class Reduce:
        def __init__(self, spans, own, term, landing, total, inbox, relay, acc, sems):
            self.spans = spans
            self.own, self.term, self.landing, self.total = own, term, landing, total
            self.inbox, self.relayed, self.acc = inbox, relay, acc
            self.pair_send, self.pair_recv, self.send, self.recv, self.relay_recv = sems

        def dest(self, at):
            return pick(z, line.column(line.reduce, at))

        def pair(self, at, span, sem):
            return remote(
                self.term.at[at, span], self.landing.at[at, span], self.pair_send.at[sem], self.pair_recv.at[sem], partner
            )

        def straight(self, p, at, source=None):
            sem = p * n_z
            source = z if source is None else source
            return remote(
                self.total.at[at, self.spans[p]], self.inbox.at[source, self.spans[p]],
                self.send.at[sem + at], self.recv.at[sem + source], chip_peer(self.dest(at)),
            )

        def aside(self, p, at):
            return remote(
                self.total.at[at, self.spans[p]], self.relayed.at[self.spans[p]],
                self.send.at[p * n_z + at], self.relay_recv.at[p], chip_peer(neighbour),
            )

        def consumer(self, at):
            return flag(z, [line.consumes(c, line.reduce[c][at]) for c in range(n_z)])

        def both(self, at, span):
            return self.own[at % slots, span] + self.landing[at, span].astype(wide)

        def begin(self, at, span, sem):
            copy = self.pair(at, span, sem)
            copy.start()
            pending.append((True, [copy]))

        def finish(self, at, span, sem):
            self.pair(at, span, sem).wait_recv()
            if at == n_z - 1:
                self.acc[span] = self.both(at, span)
            else:
                self.total[at, span] = self.both(at, span).astype(low)

        def push(self, p, at):
            if at == n_z - 1:
                return
            origin = flag(z, [line.ends(c, line.reduce[c][at]) for c in range(n_z)])

            def out():
                if origin is not False:
                    when(origin, self.aside(p, at).start)
                otherwise(origin, self.straight(p, at).start)

            otherwise(self.consumer(at), out)
            pending.append((True, [self.straight(p, at)]))

        def relay(self, p):
            span = self.spans[p]
            for at in range(n_z - 1):

                def out():
                    self.aside(p, at).wait_recv()
                    self.total[at, span] = (self.both(at, span) + self.relayed[span].astype(wide)).astype(low)
                    self.straight(p, at).start()

                when(self.consumer(at), out)

        def collect(self, p):
            span = self.spans[p]
            for at in range(n_z - 1):
                source = pick(z, line.column(line.near, at))
                ok = flag(z, [not line.ends(c, line.near[c][at]) for c in range(n_z)])

                def add():
                    self.straight(p, 0, source).wait_recv()
                    self.acc[span] += self.inbox[source, span].astype(wide)

                when(ok, add)

    def spans_of(size, tail):
        return [pl.ds(p * size, size + (tail if p == pieces - 1 else 0)) for p in range(pieces)]

    key_fill = pieces * tokens + rope_width
    key_all = pl.ds(0, key_fill)
    key_set = Reduce(
        spans_of(tokens, rope_width), own_k, term_k, pair_k, sum_k, in_k, relay_k, acc_k,
        (kp_send, kp_recv, kz_send, kz_recv, kr_recv),
    )

    def key_terms(at):
        dest = key_set.dest(at)
        keys = pl.ds(pl.multiple_of(dest * chip_rows, chip_rows), chip_rows)
        scale = factor[dest]
        expo[keys, :] = (expo[keys, :].astype(wide) * scale).astype(low)
        slope[keys, :] = (slope[keys, :].astype(wide) * (scale * softmax_scale)).astype(low)
        value = dot(expo[keys, :], grad[...], 1, 0) + dot(slope[keys, :], ql[...], 1, 0)
        rope = dot(qr2t[...], slope[keys, :], 1, 1)
        rope = rope[:rope_width] + rope[rope_width:]
        for c in range(2):
            for p in range(pieces):
                key_stage[c, p * tokens : (p + 1) * tokens, :] = value[
                    c * tokens : (c + 1) * tokens, p * lanes : (p + 1) * lanes
                ]
            key_stage[c, pieces * tokens :, :] = rope[:, c * tokens : (c + 1) * tokens]
        own_k[at % slots] = key_stage[core]
        term_k[at] = key_stage[other].astype(low)

    def key_steps():
        for at in range(n_z + lag):
            if at < n_z:
                key_terms(at)
                key_set.begin(at, key_all, at)
            if at >= lag:
                key_set.finish(at - lag, key_all, at - lag)
                key_set.push(0, at - lag)

    def push_keys(p):
        for at in range(n_z - 1):
            key_set.push(p, at)

    def query_tile(i, carry):
        span = pl.ds(pl.multiple_of(i * tile, tile), tile)
        piece = slope[:, span]
        all_lat = lat_all[...].reshape(n_ctx * tokens, latent)
        dql_ref[span, :] = dot(piece, all_lat, 0, 0).astype(low)
        qrf[span, :] = dot(piece, kr2[...], 0, 0)
        return carry

    def query_terms(step):
        count = rows // tile
        middle = count // 2
        lax.fori_loop(0 if step == 0 else middle, middle if step == 0 else count, query_tile, 0)
        if step == 0:
            return
        for at in range(heads // 2):
            even = qrf[pl.ds(2 * at, tokens, stride=heads), :]
            odd = qrf[pl.ds(2 * at + 1, tokens, stride=heads), :]
            piece = jnp.where(lower, even, odd).T.astype(low)
            dqr_ref[2 * at] = piece[:rope_width]
            dqr_ref[2 * at + 1] = piece[rope_width:]

    shared = []

    def spread_keys(p):
        span = key_set.spans[p]
        message[span] = acc_k[span].astype(low)
        landed[dp, span] = message[span]
        copies = []
        for k in range(1, n_dp):
            sem = p * n_dp + k
            copy = remote(message.at[span], landed.at[dp, span], dp_send.at[sem], dp_recv.at[sem], dp_peer(k))
            copy.start()
            copies.append(copy)
        pending.append((True, copies))
        shared.append(copies)
        dlat_ref[:, p * lanes : (p + 1) * lanes] = message[p * tokens : (p + 1) * tokens]
        if p == pieces - 1:
            drope_ref[...] = message[pieces * tokens :]

    packed = height % 32 == 0
    rope_rows = height // 2 if packed else padded
    down_set = Reduce(
        spans_of(padded, rope_rows), own_d, term_d, pair_d, sum_d, in_d, relay_d, acc_d,
        (gp_send, gp_recv, gz_send, gz_recv, gr_recv),
    )

    def down_piece(p, index):
        every = landed[:, p * tokens : (p + 1) * tokens, :].reshape(batch * tokens, lanes)
        lat = dot(turned[index], every, 1, 0)
        if p < pieces - 1:
            return lat
        if packed:
            rope = dot(turned[index, : height // 2], rope_lo[...], 1, 1)
            rope = rope + dot(turned[index, height // 2 :], rope_hi[...], 1, 1)
        else:
            rope = dot(turned[index], rope_lo[...], 1, 1)
        return jnp.concatenate([lat, rope], axis=0)

    def down_terms(p):
        for copy in shared[p]:
            copy.wait_recv()
        if p == pieces - 1:
            for b in range(batch):
                piece = landed[b, pieces * tokens :, :]
                cols = slice(b * tokens, (b + 1) * tokens)
                rope_lo[:rope_width, cols] = piece
                rope_hi[rope_width:, cols] = piece
            rope_lo[rope_width:, :] = jnp.zeros((rope_width, batch * tokens), low)
            rope_hi[:rope_width, :] = jnp.zeros((rope_width, batch * tokens), low)
        span = down_set.spans[p]
        for at in range(n_z + lag):
            if at < n_z:
                dest = down_set.dest(at)
                term_d[at, span] = down_piece(p, dest * 2 + other).astype(low)
                down_set.begin(at, span, p * n_z + at)
                own_d[at % slots, span] = down_piece(p, dest * 2 + core)
            if at >= lag:
                down_set.finish(at - lag, span, p * n_z + at - lag)
                down_set.push(p, at - lag)

    key_steps()
    push_keys(1)
    key_set.relay(0)
    push_keys(2)
    query_terms(0)
    key_set.relay(1)
    push_keys(3)
    key_set.collect(0)
    spread_keys(0)
    pair_values()
    key_set.relay(2)
    key_set.collect(1)
    spread_keys(1)
    query_terms(1)
    start_values()
    key_set.relay(3)
    down_terms(0)
    key_set.collect(2)
    spread_keys(2)
    key_set.collect(3)
    spread_keys(3)
    down_terms(1)
    down_set.relay(0)
    down_terms(2)
    down_set.relay(1)
    down_terms(3)
    down_set.relay(2)
    down_set.relay(3)
    for k in range(1, n_z):
        value_sends[k - 1].wait_recv()
        uv_ref[...] += val_in[k].astype(wide)
    for p in range(pieces):
        down_set.collect(p)
        down_ref[:, p * lanes : (p + 1) * lanes] = acc_d[p * padded : p * padded + height]
    rope = acc_d[pieces * padded :]
    if packed:
        down_ref[: height // 2, latent:] = rope[:, :rope_width]
        down_ref[height // 2 :, latent:] = rope[:, rope_width:]
    else:
        down_ref[:, latent:] = rope[:height, :rope_width]

    for ok, copies in pending:
        when(ok, functools.partial(send_waits, copies))


def store_kernel(n, *refs):
    sem = refs[2 * n]
    copies = [pltpu.make_async_copy(refs[at], refs[n + at], sem.at[at]) for at in range(n)]
    for copy in copies:
        copy.start()
    for copy in copies:
        copy.wait()


def body(n_dp, n_ctx, layer_input, kv_latent, key_rope, q_latent, q_rope, saved_output, w_uv, d_out, blocks):
    tokens = kv_latent.shape[1]
    heads, latent = q_latent.shape[2], q_latent.shape[3]
    rope_width = key_rope.shape[2]
    rows = tokens * heads
    seq_rows = tokens * n_ctx
    n_z = n_ctx // 2
    values = w_uv.shape[1]
    batch, _, width = layer_input.shape
    height = width // n_ctx
    padded = -(-height // 16) * 16
    down_fill = 4 * padded + (height // 2 if height % 32 == 0 else padded)
    key_fill = 4 * tokens + rope_width
    pieces = 4
    share = latent // (n_dp * n_ctx)
    two = 2 * rope_width
    vmem = pl.BlockSpec(memory_space=pltpu.VMEM)
    hbm = pl.BlockSpec(memory_space=pltpu.HBM)
    dma = lambda n: pltpu.SemaphoreType.DMA((n,))

    def stage(fill):
        half = lambda *dims: pltpu.VMEM((*dims, fill, 128), low)
        return [
            pltpu.VMEM((4, fill, 128), wide), half(n_z), half(n_z), half(n_z), half(n_z), half(),
            pltpu.VMEM((fill, 128), wide),
        ]

    outs = (
        ((rows, latent), low),
        ((heads, rope_width, tokens), low),
        ((tokens, latent), low),
        ((rope_width, tokens), low),
        ((height, latent + rope_width), wide),
        ((share, values), wide),
    )
    found = pl.pallas_call(
        functools.partial(main_kernel, n_dp, n_ctx),
        out_shape=tuple(pltpu.VMEM(shape, kind) for shape, kind in outs),
        in_specs=[pl.BlockSpec(memory_space=pltpu.SMEM)] + [hbm] * 8,
        out_specs=(vmem,) * 6,
        scratch_shapes=[
            pltpu.VMEM((n_ctx, tokens, latent), low),
            pltpu.VMEM((n_ctx, rope_width, tokens), low),
            pltpu.VMEM((seq_rows, two), low),
            pltpu.VMEM((rows, latent), low),
            pltpu.VMEM((heads, rope_width, tokens), low),
            pltpu.VMEM((rows, two), wide),
            pltpu.VMEM((rows, two), low),
            pltpu.VMEM((two, rows), low),
            pltpu.VMEM((rows, latent), low),
            pltpu.VMEM((latent, values), low),
            pltpu.VMEM((tokens, values), low),
            pltpu.VMEM(layer_input.shape, low),
            pltpu.VMEM((n_ctx, padded, batch * tokens), low),
            pltpu.VMEM((rows, values), low),
            pltpu.VMEM((rows, latent), low),
            pltpu.VMEM((1, rows), wide),
            pltpu.VMEM((seq_rows, 1), jnp.int32),
            pltpu.VMEM((seq_rows, rows), low),
            pltpu.VMEM((seq_rows, rows), low),
            pltpu.VMEM((n_z, 1, rows), wide),
            pltpu.VMEM((n_z, 1, rows), wide),
            pltpu.VMEM((n_z, 1, rows), wide),
            pltpu.VMEM((n_dp, latent // n_dp, values), low),
            pltpu.VMEM((n_dp, latent // n_dp, values), low),
            pltpu.VMEM((n_ctx, share, values), wide),
            pltpu.VMEM((n_z, share, values), low),
            pltpu.VMEM((n_z, share, values), low),
            pltpu.VMEM((n_z, share, values), low),
            pltpu.VMEM((n_z, share, values), low),
            pltpu.VMEM((2, key_fill, 128), wide),
            *stage(key_fill),
            pltpu.VMEM((key_fill, 128), low),
            pltpu.VMEM((n_dp, key_fill, 128), low),
            *stage(down_fill),
            pltpu.VMEM((two, batch * tokens), low),
            pltpu.VMEM((two, batch * tokens), low),
            dma(8), dma(3 * n_z), dma(3 * n_z), dma(3 * n_z), dma(3 * n_z), dma(3 * n_z),
            dma(n_dp), dma(n_dp), dma(n_z), dma(n_z), dma(n_z), dma(n_z),
            dma(n_z), dma(n_z), dma(pieces * n_z), dma(pieces * n_z), dma(pieces),
            dma(pieces * n_z), dma(pieces * n_z), dma(pieces * n_z), dma(pieces * n_z), dma(pieces),
            dma(pieces * n_dp), dma(pieces * n_dp),
        ],
        compiler_params=pltpu.CompilerParams(
            collective_id=0, has_side_effects=True, vmem_limit_bytes=VMEM_LIMIT
        ),
        name="main",
    )(
        blocks, kv_latent[0], key_rope[0].T,
        q_latent[0].reshape(rows, latent), jnp.transpose(q_rope[0], (1, 2, 0)),
        saved_output[0].reshape(rows, latent), w_uv, d_out[0], layer_input,
    )
    d_lat, d_rope, k_lat, k_rope, grad_down, grad_uv = pl.pallas_call(
        functools.partial(store_kernel, len(outs)),
        out_shape=tuple(jax.ShapeDtypeStruct(shape, kind) for shape, kind in outs),
        in_specs=[vmem] * len(outs),
        out_specs=(hbm,) * len(outs),
        scratch_shapes=[dma(len(outs))],
        compiler_params=pltpu.CompilerParams(vmem_limit_bytes=4 * 1024 * 1024),
        name="store",
    )(*found)
    return (
        d_lat.reshape(1, tokens, heads, latent),
        jnp.transpose(d_rope, (2, 0, 1))[None],
        k_lat[None],
        k_rope.T[None],
        grad_down,
        grad_uv,
    )


def solution(mesh):
    n_dp, n_ctx = mesh.shape["dp"], mesh.shape["ctx"]
    in_specs = (
        P(None, "ctx", "dp"),
        P("dp", "ctx", None),
        P("dp", "ctx", None),
        P("dp", "ctx", None, None),
        P("dp", "ctx", None, None),
        P("dp", "ctx", None, None),
        P(),
        P("dp", "ctx", None),
        P(),
    )
    out_specs = (
        P("dp", "ctx", None, None),
        P("dp", "ctx", None, None),
        P("dp", "ctx", None),
        P("dp", "ctx", None),
        P(("dp", "ctx"), None),
        P(("dp", "ctx"), None),
    )
    return jax.shard_map(
        functools.partial(body, n_dp, n_ctx),
        mesh=mesh, in_specs=in_specs, out_specs=out_specs, check_vma=False,
    )
```

```python
import functools
import math

import jax
import jax.numpy as jnp
from jax import lax
from jax.experimental import pallas as pl
from jax.experimental.pallas import tpu as pltpu
from jax.sharding import PartitionSpec as P

softmax_scale = 1.0 / math.sqrt(192.0)
score_scale = softmax_scale / math.log(2.0)
hidden_score = -1e30
wide = jnp.float32
low = jnp.bfloat16
MESH = pl.DeviceIdType.MESH
VMEM_LIMIT = 58 * 1024 * 1024
HYBRID = True


def dot(a, b, ca, cb):
    return lax.dot_general(a, b, (((ca,), (cb,)), ((), ())), preferred_element_type=wide)


def remote(src, dst, send, recv, peer):
    return pltpu.make_async_remote_copy(
        src_ref=src, dst_ref=dst, send_sem=send, recv_sem=recv, device_id=peer, device_id_type=MESH
    )


def pick(z, values):
    values = [int(v) for v in values]
    if all(v == values[0] for v in values):
        return values[0]
    out = values[0]
    for at, v in enumerate(values[1:], 1):
        out = jnp.where(z == at, v, out)
    return out


def flag(z, values):
    values = [bool(v) for v in values]
    if all(values) or not any(values):
        return values[0]
    return pick(z, values) == 1


def when(condition, action):
    if condition is True:
        action()
    elif condition is not False:
        pl.when(condition)(action)


def otherwise(condition, action):
    if condition is False:
        action()
    elif condition is not True:
        pl.when(jnp.logical_not(condition))(action)


class Line:
    def __init__(self, n):
        self.n, self.hybrid = n, HYBRID and n >= 4
        far = lambda z: sorted([d for d in range(n) if d != z], key=lambda d: (-abs(d - z), d))
        self.near = [sorted([d for d in range(n) if d != z], key=lambda d: (abs(d - z), d)) for z in range(n)]
        first = lambda z: [d for d in self.near[z] if self.forwards(z, d)]
        self.arrive = [first(z) + [d for d in self.near[z] if d not in first(z)] for z in range(n)]
        self.gather = [[d for d in far(z) if not self.ends(z, d)] + [d for d in far(z) if self.ends(z, d)] for z in range(n)]
        self.reduce = []
        for z in range(n):
            order = far(z)
            relayed = [d for d in order if self.consumes(z, d)]
            self.reduce.append([d for d in order if d not in relayed] + relayed + [z])

    def ends(self, z, d):
        return self.hybrid and {z, d} == {0, self.n - 1}

    def consumes(self, z, d):
        return self.hybrid and (z, d) in ((1, self.n - 1), (self.n - 2, 0))

    def forwards(self, z, owner):
        return self.hybrid and (z, owner) in ((1, self.n - 1), (self.n - 2, 0))

    def column(self, table, at):
        return [row[at] for row in table]


def main_kernel(
    n_dp, n_ctx,
    blocks_ref, lat_hbm, rope_hbm, ql_hbm, qr_hbm, saved_hbm, weight_hbm, out_hbm, layer_hbm,
    dql_ref, dqr_ref, dlat_ref, drope_ref, down_ref, uv_ref,
    lat_all, rope_all, kr2, ql, qrt, qrf, qr2, qr2t, saved, weight, dout, layer, turned,
    spread, grad, delta, posk, expo, slope, tops, sums, factor,
    val_parts, val_landed, val_total, val_term, val_pair, val_sum, val_in,
    key_stage, own_k, term_k, landing_k, sum_k, in_k, relay_k, acc_k, message, landed,
    own_d, term_d, pair_d, sum_d, in_d, relay_d, acc_d,
    rope_lo, rope_hi,
    local_sem, key_send, key_recv, fwd_send, fwd_recv, relay_send,
    val_send, val_recv, vp_send, vp_recv, vz_send, vz_recv,
    kp_send, kp_recv, kz_send, kz_recv, kr_recv, gp_send, gp_recv, gz_send, gz_recv, gr_recv, dp_send, dp_recv,
):
    dp, ctx = lax.axis_index("dp"), lax.axis_index("ctx")
    n_z = n_ctx // 2
    z, core = ctx // 2, ctx % 2
    other = 1 - core
    line = Line(n_z)
    partner = (dp, z * 2 + other)
    chip_peer = lambda c: (dp, c * 2 + core)
    dp_peer = lambda k: (lax.rem(dp + k, n_dp), ctx)
    tokens, latent = lat_hbm.shape
    rope_width = rope_hbm.shape[0]
    rows = ql.shape[0]
    heads = rows // tokens
    half = tokens // 2
    chip_rows = 2 * tokens
    values = dout.shape[1]
    pieces = 4
    lanes = latent // pieces

    def local(at, src, dst):
        copy = pltpu.make_async_copy(src, dst, local_sem.at[at])
        copy.start()
        return copy

    lat_in = local(0, lat_hbm, lat_all.at[ctx])
    rope_in = local(1, rope_hbm, rope_all.at[ctx])
    out_in = local(2, out_hbm, dout)
    qr_in = local(3, qr_hbm, qrt)
    saved_in = local(4, saved_hbm, saved)
    weight_in = local(5, weight_hbm, weight)
    ql_in = local(6, ql_hbm, ql)
    layer_in = local(7, layer_hbm, layer)

    peers = [partner]
    peers += [chip_peer(lax.rem(z + k, n_z)) for k in range(1, n_z)]
    peers += [dp_peer(k) for k in range(1, n_dp)]
    barrier = pltpu.get_barrier_semaphore()
    for peer in peers:
        pl.semaphore_signal(barrier, inc=1, device_id=peer, device_id_type=MESH)
    for j in range(2 * n_ctx):
        posk[j * half : (j + 1) * half, :] = blocks_ref[j] * half + lax.broadcasted_iota(jnp.int32, (half, 1), 0)
    lat_in.wait()
    rope_in.wait()
    pl.semaphore_wait(barrier, len(peers))

    def key_copies(owner, sends, recvs, recv_at, peer):
        index = owner * 2 + core
        refs = [lat_all.at[index, pl.ds(0, half)], lat_all.at[index, pl.ds(half, half)], rope_all.at[index]]
        return [
            remote(ref, ref, sends.at[n // 2], recvs.at[recv_at[n]], peer) for n, ref in enumerate(refs)
        ]

    def apart(owner):
        return [n * n_z + owner for n in range(3)]

    def key_blocks_sent(sends, count):
        for n, ref in enumerate([lat_all, rope_all]):
            blocks = ref.at[pl.ds(0, count)]
            remote(blocks, blocks, sends.at[n], key_recv.at[0], partner).wait_send()

    def start_all(copies):
        for copy in copies:
            copy.start()

    for at in range(n_z - 1):
        dest = pick(z, line.column(line.gather, at))
        ok = flag(z, [not line.ends(c, line.gather[c][at]) for c in range(n_z)])
        copies = key_copies(z, key_send, key_recv, apart(z), chip_peer(dest))
        when(ok, functools.partial(start_all, copies))
    start_all(key_copies(z, fwd_send, fwd_recv, [z] * 3, partner))

    out_in.wait()
    lane = lax.broadcasted_iota(jnp.int32, (heads, values), 1)
    head = lax.broadcasted_iota(jnp.int32, (heads, values), 0)
    keep = (lane // (values // heads) == head)[None]
    group = min(16, tokens)
    for start in range(0, tokens, group):
        piece = dout[start : start + group].astype(wide)
        piece = jnp.broadcast_to(piece[:, None, :], (group, heads, values))
        piece = jnp.where(keep, piece, 0.0).reshape(group * heads, values)
        spread[start * heads : (start + group) * heads, :] = piece.astype(low)

    qr_in.wait()
    two = 2 * rope_width
    lower = lax.broadcasted_iota(jnp.int32, (tokens, two), 1) < rope_width
    for at in range(heads // 2):
        piece = qrt[2 * at : 2 * at + 2].reshape(two, tokens).astype(wide).T
        qrf[pl.ds(2 * at, tokens, stride=heads), :] = jnp.where(lower, piece, 0.0)
        qrf[pl.ds(2 * at + 1, tokens, stride=heads), :] = jnp.where(lower, 0.0, piece)
    qr2[...] = qrf[...].astype(low)
    qr2t[...] = qrf[...].T.astype(low)

    saved_in.wait()
    share = val_parts.shape[1]
    value = dot(saved[...], spread[...], 0, 0).astype(low)
    for d in range(n_dp):
        val_parts[d] = value[d * share : (d + 1) * share]
    value_copies = []
    for k in range(1, n_dp):
        copy = remote(
            val_parts.at[lax.rem(dp + k, n_dp)], val_landed.at[k], val_send.at[0], val_recv.at[0], dp_peer(k)
        )
        copy.start()
        value_copies.append(copy)

    weight_in.wait()
    tile = min(256, rows)
    for start in range(0, rows, tile):
        piece = dot(spread[start : start + tile], weight[...], 1, 1).astype(low)
        grad[start : start + tile, :] = piece
        prod = piece.astype(wide) * saved[start : start + tile].astype(wide)
        total = prod[:, :128]
        for at in range(128, prod.shape[1], 128):
            total = total + prod[:, at : at + 128]
        delta[:, start : start + tile] = jnp.sum(total.T, axis=0, keepdims=True)
    ql_in.wait()

    low_block, high_block = blocks_ref[2 * ctx], blocks_ref[2 * ctx + 1]

    def pass_on(owner):
        start_all(key_copies(owner, fwd_send, fwd_recv, [owner] * 3, partner))

    def chunk(owner):
        remote(term_k.at[0], landing_k.at[0], fwd_send.at[0], fwd_recv.at[owner], partner).wait_recv()
        keys = pl.ds(pl.multiple_of(owner * chip_rows, chip_rows), chip_rows)
        for at in range(2):
            piece = rope_all[owner * 2 + at].astype(wide)
            kr2[pl.ds(pl.multiple_of((owner * 2 + at) * tokens, tokens), tokens), :] = (
                jnp.concatenate([piece, piece], axis=0).T.astype(low)
            )

        def score_tile(i, carry):
            if isinstance(i, int):
                span = pl.ds(i * tile, tile)
            else:
                span = pl.ds(pl.multiple_of(i * tile, tile), tile)
            key_lat = lat_all[pl.ds(owner * 2, 2)].reshape(chip_rows, latent)
            scores = dot(key_lat, ql[span, :], 1, 1) + dot(kr2[keys, :], qr2[span, :], 1, 1)
            token = (i * tile + lax.broadcasted_iota(jnp.int32, (1, tile), 1)) // heads
            posq = jnp.where(token < half, low_block * half + token, high_block * half + token - half)
            scores = jnp.where(posk[keys, :] <= posq, scores * score_scale, hidden_score)
            top = jnp.max(scores, axis=0, keepdims=True)
            piece = jnp.exp2(scores - top)
            tops[owner, :, span] = top
            sums[owner, :, span] = jnp.sum(piece, axis=0, keepdims=True)
            expo[keys, span] = piece.astype(low)
            grad_prob = dot(key_lat, grad[span, :], 1, 1)
            slope[keys, span] = (piece * (grad_prob - delta[:, span])).astype(low)
            return carry

        if n_z <= 4:
            for i in range(rows // tile):
                score_tile(i, 0)
        else:
            lax.fori_loop(0, rows // tile, score_tile, 0)

    chunk(z)

    height = down_ref.shape[0]
    padded = turned.shape[1]
    batch = layer.shape[0]

    def turn():
        layer_in.wait()
        for d in range(batch):
            piece = layer[d].T
            for c in range(n_ctx):
                rows_c = piece[c * height : (c + 1) * height]
                if padded > height:
                    rows_c = jnp.concatenate(
                        [rows_c.astype(wide), jnp.zeros((padded - height, tokens), wide)], axis=0
                    ).astype(low)
                turned[c, :, d * tokens : (d + 1) * tokens] = rows_c

    value_pairs, value_sends = [], []

    def pair_values():
        others = pl.ds(1, n_dp - 1)
        remote(val_parts.at[others], val_landed.at[others], val_send.at[0], val_recv.at[0], partner).wait_recv()
        total = val_parts[dp].astype(wide)
        for k in range(1, n_dp):
            total = total + val_landed[k].astype(wide)
        piece = val_total.shape[1]
        for c in range(n_ctx):
            val_total[c] = total[c * piece : (c + 1) * piece]
        for k in range(n_z):
            dest = lax.rem(z + k, n_z)
            val_term[k] = val_total[dest * 2 + other].astype(low)
            copy = remote(val_term.at[k], val_pair.at[k], vp_send.at[0], vp_recv.at[0], partner)
            copy.start()
            value_pairs.append(copy)

    def start_values():
        remote(val_term, val_pair, vp_send.at[0], vp_recv.at[0], partner).wait_recv()
        for k in list(range(1, n_z)) + [0]:
            dest = lax.rem(z + k, n_z)
            added = val_total[dest * 2 + core] + val_pair[k].astype(wide)
            if k == 0:
                uv_ref[...] = added
            else:
                val_sum[k] = added.astype(low)
                copy = remote(val_sum.at[k], val_in.at[k], vz_send.at[0], vz_recv.at[0], chip_peer(dest))
                copy.start()
                value_sends.append(copy)

    for at in range(n_z - 1):
        owner = pick(z, line.column(line.arrive, at))
        relay_ok = flag(z, [line.forwards(c, line.arrive[c][at]) for c in range(n_z)])
        copies = []
        if relay_ok is not False:
            end = jnp.where(z == 1, 0, n_z - 1)
            copies = key_copies(owner, relay_send, key_recv, apart(owner), chip_peer(end))
        for n, copy in enumerate(key_copies(owner, key_send, key_recv, apart(owner), partner)):
            copy.wait_recv()
            if copies:
                when(relay_ok, copies[n].start)
        pass_on(owner)
        chunk(owner)
        if at == max(n_z - 3, 0):
            turn()

    top = tops[0]
    for c in range(1, n_z):
        top = jnp.maximum(top, tops[c])
    total = jnp.zeros_like(top)
    for c in range(n_z):
        weight_c = jnp.exp2(tops[c] - top)
        factor[c] = weight_c
        total = total + sums[c] * weight_c
    inverse = 1.0 / total
    for c in range(n_z):
        factor[c] = factor[c] * inverse

    lag, slots = 2, 4
    neighbour = jnp.where(z == 0, 1, n_z - 2)
    at_end = flag(z, [line.hybrid and c in (0, n_z - 1) for c in range(n_z)])

    class Reduce:
        def __init__(self, spans, own, term, landing, total, inbox, relay, acc, sems):
            self.spans = spans
            self.own, self.term, self.landing, self.total = own, term, landing, total
            self.inbox, self.relayed, self.acc = inbox, relay, acc
            self.pair_send, self.pair_recv, self.send, self.recv, self.relay_recv = sems

        def dest(self, at):
            return pick(z, line.column(line.reduce, at))

        def pair(self, at, span, sem):
            return remote(
                self.term.at[at, span], self.landing.at[at, span], self.pair_send.at[0], self.pair_recv.at[sem], partner
            )

        def straight(self, p, at):
            return remote(
                self.total.at[at, self.spans[p]], self.inbox.at[z, self.spans[p]],
                self.send.at[0], self.recv.at[p], chip_peer(self.dest(at)),
            )

        def aside(self, p, at):
            return remote(
                self.total.at[at, self.spans[p]], self.relayed.at[self.spans[p]],
                self.send.at[0], self.relay_recv.at[p], chip_peer(neighbour),
            )

        def consumer(self, at):
            return flag(z, [line.consumes(c, line.reduce[c][at]) for c in range(n_z)])

        def both(self, at, span):
            return self.own[at % slots, span] + self.landing[at, span].astype(wide)

        def begin(self, at, span, sem):
            self.pair(at, span, sem).start()

        def finish(self, at, span, sem):
            self.pair(at, span, sem).wait_recv()
            if at == n_z - 1:
                self.acc[span] = self.both(at, span)
            else:
                self.total[at, span] = self.both(at, span).astype(low)

        def push(self, p, at):
            if at == n_z - 1:
                return
            origin = flag(z, [line.ends(c, line.reduce[c][at]) for c in range(n_z)])

            def out():
                if origin is not False:
                    when(origin, self.aside(p, at).start)
                otherwise(origin, self.straight(p, at).start)

            otherwise(self.consumer(at), out)

        def relay(self, p):
            span = self.spans[p]
            for at in range(n_z - 1):

                def out():
                    self.aside(p, at).wait_recv()
                    self.total[at, span] = (self.both(at, span) + self.relayed[span].astype(wide)).astype(low)
                    self.straight(p, at).start()

                when(self.consumer(at), out)

        def collect(self, p):
            span = self.spans[p]

            def arrived(count):
                blocks = pl.ds(0, count)
                remote(
                    self.total.at[blocks, span], self.inbox.at[blocks, span],
                    self.send.at[0], self.recv.at[p], partner,
                ).wait_recv()

            when(at_end, functools.partial(arrived, n_z - 2))
            otherwise(at_end, functools.partial(arrived, n_z - 1))
            for at in range(n_z - 1):
                source = pick(z, line.column(line.near, at))
                ok = flag(z, [not line.ends(c, line.near[c][at]) for c in range(n_z)])

                def add():
                    self.acc[span] += self.inbox[source, span].astype(wide)

                when(ok, add)

        def sent(self):
            blocks = pl.ds(0, n_z - 1)
            remote(self.term, self.landing, self.pair_send.at[0], self.pair_recv.at[0], partner).wait_send()
            remote(
                self.total.at[blocks], self.inbox.at[blocks], self.send.at[0], self.recv.at[0], partner
            ).wait_send()

    def spans_of(size, tail):
        return [pl.ds(p * size, size + (tail if p == pieces - 1 else 0)) for p in range(pieces)]

    key_fill = pieces * tokens + rope_width
    key_all = pl.ds(0, key_fill)
    key_set = Reduce(
        spans_of(tokens, rope_width), own_k, term_k, landing_k, sum_k, in_k, relay_k, acc_k,
        (kp_send, kp_recv, kz_send, kz_recv, kr_recv),
    )

    def key_terms(at):
        dest = key_set.dest(at)
        keys = pl.ds(pl.multiple_of(dest * chip_rows, chip_rows), chip_rows)
        scale = factor[dest]
        expo[keys, :] = (expo[keys, :].astype(wide) * scale).astype(low)
        slope[keys, :] = (slope[keys, :].astype(wide) * (scale * softmax_scale)).astype(low)
        value = dot(expo[keys, :], grad[...], 1, 0) + dot(slope[keys, :], ql[...], 1, 0)
        rope = dot(qr2t[...], slope[keys, :], 1, 1)
        rope = rope[:rope_width] + rope[rope_width:]
        for c in range(2):
            for p in range(pieces):
                key_stage[c, p * tokens : (p + 1) * tokens, :] = value[
                    c * tokens : (c + 1) * tokens, p * lanes : (p + 1) * lanes
                ]
            key_stage[c, pieces * tokens :, :] = rope[:, c * tokens : (c + 1) * tokens]
        own_k[at % slots] = key_stage[core]
        term_k[at] = key_stage[other].astype(low)

    def key_steps():
        for at in range(n_z + 1):
            if at < n_z:
                key_terms(at)
                key_set.begin(at, key_all, at)
            if at >= 1:
                key_set.finish(at - 1, key_all, at - 1)
                key_set.push(0, at - 1)

    def push_keys(p):
        for at in range(n_z - 1):
            key_set.push(p, at)

    def query_tile(i, carry):
        span = pl.ds(pl.multiple_of(i * tile, tile), tile)
        piece = slope[:, span]
        all_lat = lat_all[...].reshape(n_ctx * tokens, latent)
        dql_ref[span, :] = dot(piece, all_lat, 0, 0).astype(low)
        qrf[span, :] = dot(piece, kr2[...], 0, 0)
        return carry

    def query_terms(step):
        count = rows // tile
        middle = count // 2
        lax.fori_loop(0 if step == 0 else middle, middle if step == 0 else count, query_tile, 0)
        if step == 0:
            return
        for at in range(heads // 2):
            even = qrf[pl.ds(2 * at, tokens, stride=heads), :]
            odd = qrf[pl.ds(2 * at + 1, tokens, stride=heads), :]
            piece = jnp.where(lower, even, odd).T.astype(low)
            dqr_ref[2 * at] = piece[:rope_width]
            dqr_ref[2 * at + 1] = piece[rope_width:]

    def spread_keys(p):
        span = key_set.spans[p]
        message[span] = acc_k[span].astype(low)
        landed[dp, span] = message[span]
        for k in range(1, n_dp):
            remote(
                message.at[span], landed.at[dp, span], dp_send.at[0], dp_recv.at[p], dp_peer(k)
            ).start()
        dlat_ref[:, p * lanes : (p + 1) * lanes] = message[p * tokens : (p + 1) * tokens]
        if p == pieces - 1:
            drope_ref[...] = message[pieces * tokens :]

    packed = height % 32 == 0
    rope_rows = height // 2 if packed else padded
    down_set = Reduce(
        spans_of(padded, rope_rows), own_d, term_d, pair_d, sum_d, in_d, relay_d, acc_d,
        (gp_send, gp_recv, gz_send, gz_recv, gr_recv),
    )

    def down_piece(p, index):
        every = landed[:, p * tokens : (p + 1) * tokens, :].reshape(batch * tokens, lanes)
        lat = dot(turned[index], every, 1, 0)
        if p < pieces - 1:
            return lat
        if packed:
            rope = dot(turned[index, : height // 2], rope_lo[...], 1, 1)
            rope = rope + dot(turned[index, height // 2 :], rope_hi[...], 1, 1)
        else:
            rope = dot(turned[index], rope_lo[...], 1, 1)
        return jnp.concatenate([lat, rope], axis=0)

    def down_terms(p):
        others = pl.ds(0, n_dp - 1)
        arrived = landed.at[others, key_set.spans[p]]
        remote(arrived, arrived, dp_send.at[0], dp_recv.at[p], partner).wait_recv()
        if p == pieces - 1:
            for b in range(batch):
                piece = landed[b, pieces * tokens :, :]
                cols = slice(b * tokens, (b + 1) * tokens)
                rope_lo[:rope_width, cols] = piece
                rope_hi[rope_width:, cols] = piece
            rope_lo[rope_width:, :] = jnp.zeros((rope_width, batch * tokens), low)
            rope_hi[:rope_width, :] = jnp.zeros((rope_width, batch * tokens), low)
        span = down_set.spans[p]
        for at in range(n_z + lag):
            if at < n_z:
                dest = down_set.dest(at)
                term_d[at, span] = down_piece(p, dest * 2 + other).astype(low)
                down_set.begin(at, span, p * n_z + at)
                own_d[at % slots, span] = down_piece(p, dest * 2 + core)
            if at >= lag:
                down_set.finish(at - lag, span, p * n_z + at - lag)
                down_set.push(p, at - lag)

    key_steps()
    push_keys(1)
    key_set.relay(0)
    push_keys(2)
    query_terms(0)
    key_set.relay(1)
    push_keys(3)
    key_set.collect(0)
    spread_keys(0)
    pair_values()
    key_set.relay(2)
    key_set.collect(1)
    spread_keys(1)
    query_terms(1)
    start_values()
    key_set.relay(3)
    down_terms(0)
    key_set.collect(2)
    spread_keys(2)
    key_set.collect(3)
    spread_keys(3)
    down_terms(1)
    down_set.relay(0)
    down_terms(2)
    down_set.relay(1)
    down_terms(3)
    down_set.relay(2)
    down_set.relay(3)
    others = pl.ds(1, n_z - 1)
    remote(val_sum.at[others], val_in.at[others], vz_send.at[0], vz_recv.at[0], partner).wait_recv()
    for k in range(1, n_z):
        uv_ref[...] += val_in[k].astype(wide)
    for p in range(pieces):
        down_set.collect(p)
        down_ref[:, p * lanes : (p + 1) * lanes] = acc_d[p * padded : p * padded + height]
    rope = acc_d[pieces * padded :]
    if packed:
        down_ref[: height // 2, latent:] = rope[:, :rope_width]
        down_ref[height // 2 :, latent:] = rope[:, rope_width:]
    else:
        down_ref[:, latent:] = rope[:height, :rope_width]

    when(at_end, functools.partial(key_blocks_sent, key_send, n_z - 2))
    otherwise(at_end, functools.partial(key_blocks_sent, key_send, n_z - 1))
    key_blocks_sent(fwd_send, n_z)
    relays = flag(z, [line.hybrid and c in (1, n_z - 2) for c in range(n_z)])
    when(relays, functools.partial(key_blocks_sent, relay_send, 1))
    others = pl.ds(0, n_dp - 1)
    remote(val_parts.at[others], val_landed.at[others], val_send.at[0], val_recv.at[0], partner).wait_send()
    remote(val_term, val_pair, vp_send.at[0], vp_recv.at[0], partner).wait_send()
    others = pl.ds(0, n_z - 1)
    remote(val_sum.at[others], val_in.at[others], vz_send.at[0], vz_recv.at[0], partner).wait_send()
    key_set.sent()
    down_set.sent()
    sent = landed.at[pl.ds(0, n_dp - 1)]
    remote(sent, sent, dp_send.at[0], dp_recv.at[0], partner).wait_send()


def store_kernel(n, *refs):
    sem = refs[2 * n]
    copies = []
    for at in range(n):
        rows = refs[at].shape[0]
        parts = 4 if rows % 64 == 0 and rows >= 512 else 1
        for part in range(parts):
            span = pl.ds(part * (rows // parts), rows // parts)
            copies.append(pltpu.make_async_copy(refs[at].at[span], refs[n + at].at[span], sem.at[len(copies)]))
    for copy in copies:
        copy.start()
    for copy in copies:
        copy.wait()


def body(n_dp, n_ctx, layer_input, kv_latent, key_rope, q_latent, q_rope, saved_output, w_uv, d_out, blocks):
    tokens = kv_latent.shape[1]
    heads, latent = q_latent.shape[2], q_latent.shape[3]
    rope_width = key_rope.shape[2]
    rows = tokens * heads
    seq_rows = tokens * n_ctx
    n_z = n_ctx // 2
    values = w_uv.shape[1]
    batch, _, width = layer_input.shape
    height = width // n_ctx
    padded = -(-height // 16) * 16
    down_fill = 4 * padded + (height // 2 if height % 32 == 0 else padded)
    key_fill = 4 * tokens + rope_width
    pieces = 4
    share = latent // (n_dp * n_ctx)
    two = 2 * rope_width
    vmem = pl.BlockSpec(memory_space=pltpu.VMEM)
    hbm = pl.BlockSpec(memory_space=pltpu.HBM)
    dma = lambda n: pltpu.SemaphoreType.DMA((n,))

    def stage(fill):
        half = lambda *dims: pltpu.VMEM((*dims, fill, 128), low)
        return [
            pltpu.VMEM((4, fill, 128), wide), half(n_z), half(n_z), half(n_z), half(n_z), half(),
            pltpu.VMEM((fill, 128), wide),
        ]

    outs = (
        ((rows, latent), low),
        ((heads, rope_width, tokens), low),
        ((tokens, latent), low),
        ((rope_width, tokens), low),
        ((height, latent + rope_width), wide),
        ((share, values), wide),
    )
    found = pl.pallas_call(
        functools.partial(main_kernel, n_dp, n_ctx),
        out_shape=tuple(pltpu.VMEM(shape, kind) for shape, kind in outs),
        in_specs=[pl.BlockSpec(memory_space=pltpu.SMEM)] + [hbm] * 8,
        out_specs=(vmem,) * 6,
        scratch_shapes=[
            pltpu.VMEM((n_ctx, tokens, latent), low),
            pltpu.VMEM((n_ctx, rope_width, tokens), low),
            pltpu.VMEM((seq_rows, two), low),
            pltpu.VMEM((rows, latent), low),
            pltpu.VMEM((heads, rope_width, tokens), low),
            pltpu.VMEM((rows, two), wide),
            pltpu.VMEM((rows, two), low),
            pltpu.VMEM((two, rows), low),
            pltpu.VMEM((rows, latent), low),
            pltpu.VMEM((latent, values), low),
            pltpu.VMEM((tokens, values), low),
            pltpu.VMEM(layer_input.shape, low),
            pltpu.VMEM((n_ctx, padded, batch * tokens), low),
            pltpu.VMEM((rows, values), low),
            pltpu.VMEM((rows, latent), low),
            pltpu.VMEM((1, rows), wide),
            pltpu.VMEM((seq_rows, 1), jnp.int32),
            pltpu.VMEM((seq_rows, rows), low),
            pltpu.VMEM((seq_rows, rows), low),
            pltpu.VMEM((n_z, 1, rows), wide),
            pltpu.VMEM((n_z, 1, rows), wide),
            pltpu.VMEM((n_z, 1, rows), wide),
            pltpu.VMEM((n_dp, latent // n_dp, values), low),
            pltpu.VMEM((n_dp, latent // n_dp, values), low),
            pltpu.VMEM((n_ctx, share, values), wide),
            pltpu.VMEM((n_z, share, values), low),
            pltpu.VMEM((n_z, share, values), low),
            pltpu.VMEM((n_z, share, values), low),
            pltpu.VMEM((n_z, share, values), low),
            pltpu.VMEM((2, key_fill, 128), wide),
            *stage(key_fill),
            pltpu.VMEM((key_fill, 128), low),
            pltpu.VMEM((n_dp, key_fill, 128), low),
            *stage(down_fill),
            pltpu.VMEM((two, batch * tokens), low),
            pltpu.VMEM((two, batch * tokens), low),
            dma(8), dma(2), dma(3 * n_z), dma(2), dma(n_z), dma(2),
            dma(1), dma(1), dma(1), dma(1), dma(1), dma(1),
            dma(1), dma(n_z), dma(1), dma(pieces), dma(pieces),
            dma(1), dma(pieces * n_z), dma(1), dma(pieces), dma(pieces),
            dma(1), dma(pieces),
        ],
        compiler_params=pltpu.CompilerParams(
            collective_id=0, has_side_effects=True, vmem_limit_bytes=VMEM_LIMIT
        ),
        name="main",
    )(
        blocks, kv_latent[0], key_rope[0].T,
        q_latent[0].reshape(rows, latent), jnp.transpose(q_rope[0], (1, 2, 0)),
        saved_output[0].reshape(rows, latent), w_uv, d_out[0], layer_input,
    )
    d_lat, d_rope, k_lat, k_rope, grad_down, grad_uv = pl.pallas_call(
        functools.partial(store_kernel, len(outs)),
        out_shape=tuple(jax.ShapeDtypeStruct(shape, kind) for shape, kind in outs),
        in_specs=[vmem] * len(outs),
        out_specs=(hbm,) * len(outs),
        scratch_shapes=[dma(len(outs) + 3)],
        compiler_params=pltpu.CompilerParams(vmem_limit_bytes=4 * 1024 * 1024),
        name="store",
    )(*found)
    return (
        d_lat.reshape(1, tokens, heads, latent),
        jnp.transpose(d_rope, (2, 0, 1))[None],
        k_lat[None],
        k_rope.T[None],
        grad_down,
        grad_uv,
    )


def solution(mesh):
    n_dp, n_ctx = mesh.shape["dp"], mesh.shape["ctx"]
    in_specs = (
        P(None, "ctx", "dp"),
        P("dp", "ctx", None),
        P("dp", "ctx", None),
        P("dp", "ctx", None, None),
        P("dp", "ctx", None, None),
        P("dp", "ctx", None, None),
        P(),
        P("dp", "ctx", None),
        P(),
    )
    out_specs = (
        P("dp", "ctx", None, None),
        P("dp", "ctx", None, None),
        P("dp", "ctx", None),
        P("dp", "ctx", None),
        P(("dp", "ctx"), None),
        P(("dp", "ctx"), None),
    )
    return jax.shard_map(
        functools.partial(body, n_dp, n_ctx),
        mesh=mesh, in_specs=in_specs, out_specs=out_specs, check_vma=False,
    )
```

```python
import functools
import math

import jax
import jax.numpy as jnp
from jax import lax
from jax.experimental import pallas as pl
from jax.experimental.pallas import tpu as pltpu
from jax.sharding import PartitionSpec as P

softmax_scale = 1.0 / math.sqrt(192.0)
score_scale = softmax_scale / math.log(2.0)
hidden_score = -1e30
wide = jnp.float32
low = jnp.bfloat16
MESH = pl.DeviceIdType.MESH
VMEM_LIMIT = 58 * 1024 * 1024
HYBRID = True


def dot(a, b, ca, cb):
    return lax.dot_general(a, b, (((ca,), (cb,)), ((), ())), preferred_element_type=wide)


def remote(src, dst, send, recv, peer):
    return pltpu.make_async_remote_copy(
        src_ref=src, dst_ref=dst, send_sem=send, recv_sem=recv, device_id=peer, device_id_type=MESH
    )


def pick(z, values):
    values = [int(v) for v in values]
    if all(v == values[0] for v in values):
        return values[0]
    out = values[0]
    for at, v in enumerate(values[1:], 1):
        out = jnp.where(z == at, v, out)
    return out


def flag(z, values):
    values = [bool(v) for v in values]
    if all(values) or not any(values):
        return values[0]
    return pick(z, values) == 1


def when(condition, action):
    if condition is True:
        action()
    elif condition is not False:
        pl.when(condition)(action)


def otherwise(condition, action):
    if condition is False:
        action()
    elif condition is not True:
        pl.when(jnp.logical_not(condition))(action)


class Line:
    def __init__(self, n):
        self.n, self.hybrid = n, HYBRID and n >= 4
        far = lambda z: sorted([d for d in range(n) if d != z], key=lambda d: (-abs(d - z), d))
        self.near = [sorted([d for d in range(n) if d != z], key=lambda d: (abs(d - z), d)) for z in range(n)]
        first = lambda z: [d for d in self.near[z] if self.forwards(z, d)]
        self.arrive = [first(z) + [d for d in self.near[z] if d not in first(z)] for z in range(n)]
        self.gather = [[d for d in far(z) if not self.ends(z, d)] + [d for d in far(z) if self.ends(z, d)] for z in range(n)]
        self.reduce = []
        for z in range(n):
            order = far(z)
            relayed = [d for d in order if self.consumes(z, d)]
            self.reduce.append([d for d in order if d not in relayed] + relayed + [z])

    def ends(self, z, d):
        return self.hybrid and {z, d} == {0, self.n - 1}

    def consumes(self, z, d):
        return self.hybrid and (z, d) in ((1, self.n - 1), (self.n - 2, 0))

    def forwards(self, z, owner):
        return self.hybrid and (z, owner) in ((1, self.n - 1), (self.n - 2, 0))

    def column(self, table, at):
        return [row[at] for row in table]


def main_kernel(
    n_dp, n_ctx,
    blocks_ref, lat_hbm, rope_hbm, ql_hbm, qr_hbm, saved_hbm, weight_hbm, out_hbm, layer_hbm,
    dql_ref, dqr_ref, dlat_ref, drope_ref, down_ref, uv_ref,
    lat_all, rope_all, kr2, ql, qrt, qrf, qr2, qr2t, saved, weight, dout, layer, turned,
    spread, grad, delta, posk, expo, slope, tops, sums, factor,
    val_parts, val_landed, val_total, val_term, val_pair, val_sum, val_in,
    key_stage, own_k, term_k, landing_k, sum_k, in_k, relay_k, acc_k, message, landed,
    own_d, term_d, pair_d, sum_d, in_d, relay_d, acc_d,
    rope_lo, rope_hi,
    local_sem, key_send, key_recv, fwd_send, fwd_recv, relay_send,
    val_send, val_recv, vp_send, vp_recv, vz_send, vz_recv,
    kp_send, kp_recv, kz_send, kz_recv, kr_recv, gp_send, gp_recv, gz_send, gz_recv, gr_recv, dp_send, dp_recv,
):
    dp, ctx = lax.axis_index("dp"), lax.axis_index("ctx")
    n_z = n_ctx // 2
    z, core = ctx // 2, ctx % 2
    other = 1 - core
    line = Line(n_z)
    partner = (dp, z * 2 + other)
    chip_peer = lambda c: (dp, c * 2 + core)
    dp_peer = lambda k: (lax.rem(dp + k, n_dp), ctx)
    tokens, latent = lat_hbm.shape
    rope_width = rope_hbm.shape[0]
    rows = ql.shape[0]
    heads = rows // tokens
    half = tokens // 2
    chip_rows = 2 * tokens
    values = dout.shape[1]
    pieces = 4
    lanes = latent // pieces

    def local(at, src, dst):
        copy = pltpu.make_async_copy(src, dst, local_sem.at[at])
        copy.start()
        return copy

    lat_in = local(0, lat_hbm, lat_all.at[ctx])
    rope_in = local(1, rope_hbm, rope_all.at[ctx])
    out_in = local(2, out_hbm, dout)
    qr_in = local(3, qr_hbm, qrt)
    saved_in = local(4, saved_hbm, saved)
    weight_in = local(5, weight_hbm, weight)
    ql_in = local(6, ql_hbm, ql)
    layer_in = local(7, layer_hbm, layer)

    peers = [partner]
    peers += [chip_peer(lax.rem(z + k, n_z)) for k in range(1, n_z)]
    peers += [dp_peer(k) for k in range(1, n_dp)]
    barrier = pltpu.get_barrier_semaphore()
    for peer in peers:
        pl.semaphore_signal(barrier, inc=1, device_id=peer, device_id_type=MESH)
    for j in range(2 * n_ctx):
        posk[j * half : (j + 1) * half, :] = blocks_ref[j] * half + lax.broadcasted_iota(jnp.int32, (half, 1), 0)
    lat_in.wait()
    rope_in.wait()
    pl.semaphore_wait(barrier, len(peers))

    def key_copies(owner, sends, recvs, recv_at, peer):
        index = owner * 2 + core
        refs = [lat_all.at[index, pl.ds(0, half)], lat_all.at[index, pl.ds(half, half)], rope_all.at[index]]
        return [
            remote(ref, ref, sends.at[n // 2], recvs.at[recv_at[n]], peer) for n, ref in enumerate(refs)
        ]

    def apart(owner):
        return [n * n_z + owner for n in range(3)]

    def key_blocks_sent(sends, count):
        for n, ref in enumerate([lat_all, rope_all]):
            blocks = ref.at[pl.ds(0, count)]
            remote(blocks, blocks, sends.at[n], key_recv.at[0], partner).wait_send()

    def start_all(copies):
        for copy in copies:
            copy.start()

    for at in range(n_z - 1):
        dest = pick(z, line.column(line.gather, at))
        ok = flag(z, [not line.ends(c, line.gather[c][at]) for c in range(n_z)])
        copies = key_copies(z, key_send, key_recv, apart(z), chip_peer(dest))
        when(ok, functools.partial(start_all, copies))
    start_all(key_copies(z, fwd_send, fwd_recv, [z] * 3, partner))

    out_in.wait()
    lane = lax.broadcasted_iota(jnp.int32, (heads, values), 1)
    head = lax.broadcasted_iota(jnp.int32, (heads, values), 0)
    keep = (lane // (values // heads) == head)[None]
    group = min(16, tokens)
    for start in range(0, tokens, group):
        piece = dout[start : start + group].astype(wide)
        piece = jnp.broadcast_to(piece[:, None, :], (group, heads, values))
        piece = jnp.where(keep, piece, 0.0).reshape(group * heads, values)
        spread[start * heads : (start + group) * heads, :] = piece.astype(low)

    qr_in.wait()
    two = 2 * rope_width
    lower = lax.broadcasted_iota(jnp.int32, (tokens, two), 1) < rope_width
    for at in range(heads // 2):
        piece = qrt[2 * at : 2 * at + 2].reshape(two, tokens).astype(wide).T
        qrf[pl.ds(2 * at, tokens, stride=heads), :] = jnp.where(lower, piece, 0.0)
        qrf[pl.ds(2 * at + 1, tokens, stride=heads), :] = jnp.where(lower, 0.0, piece)
    qr2[...] = qrf[...].astype(low)
    qr2t[...] = qrf[...].T.astype(low)

    saved_in.wait()
    share = val_parts.shape[1]
    value = dot(saved[...], spread[...], 0, 0).astype(low)
    for d in range(n_dp):
        val_parts[d] = value[d * share : (d + 1) * share]
    value_copies = []
    for k in range(1, n_dp):
        copy = remote(
            val_parts.at[lax.rem(dp + k, n_dp)], val_landed.at[k], val_send.at[0], val_recv.at[0], dp_peer(k)
        )
        copy.start()
        value_copies.append(copy)

    weight_in.wait()
    tile = min(256, rows)
    for start in range(0, rows, tile):
        piece = dot(spread[start : start + tile], weight[...], 1, 1).astype(low)
        grad[start : start + tile, :] = piece
        prod = piece.astype(wide) * saved[start : start + tile].astype(wide)
        total = prod[:, :128]
        for at in range(128, prod.shape[1], 128):
            total = total + prod[:, at : at + 128]
        delta[:, start : start + tile] = jnp.sum(total.T, axis=0, keepdims=True)
    ql_in.wait()

    low_block, high_block = blocks_ref[2 * ctx], blocks_ref[2 * ctx + 1]

    def pass_on(owner):
        start_all(key_copies(owner, fwd_send, fwd_recv, [owner] * 3, partner))

    def chunk(owner):
        remote(term_k.at[0], landing_k.at[0], fwd_send.at[0], fwd_recv.at[owner], partner).wait_recv()
        keys = pl.ds(pl.multiple_of(owner * chip_rows, chip_rows), chip_rows)
        for at in range(2):
            piece = rope_all[owner * 2 + at].astype(wide)
            kr2[pl.ds(pl.multiple_of((owner * 2 + at) * tokens, tokens), tokens), :] = (
                jnp.concatenate([piece, piece], axis=0).T.astype(low)
            )

        def score_tile(i, carry):
            if isinstance(i, int):
                span = pl.ds(i * tile, tile)
            else:
                span = pl.ds(pl.multiple_of(i * tile, tile), tile)
            key_lat = lat_all[pl.ds(owner * 2, 2)].reshape(chip_rows, latent)
            scores = dot(key_lat, ql[span, :], 1, 1) + dot(kr2[keys, :], qr2[span, :], 1, 1)
            token = (i * tile + lax.broadcasted_iota(jnp.int32, (1, tile), 1)) // heads
            posq = jnp.where(token < half, low_block * half + token, high_block * half + token - half)
            scores = jnp.where(posk[keys, :] <= posq, scores * score_scale, hidden_score)
            top = jnp.max(scores, axis=0, keepdims=True)
            piece = jnp.exp2(scores - top)
            tops[owner, :, span] = top
            sums[owner, :, span] = jnp.sum(piece, axis=0, keepdims=True)
            expo[keys, span] = piece.astype(low)
            grad_prob = dot(key_lat, grad[span, :], 1, 1)
            slope[keys, span] = (piece * (grad_prob - delta[:, span])).astype(low)
            return carry

        if n_z <= 4:
            for i in range(rows // tile):
                score_tile(i, 0)
        else:
            lax.fori_loop(0, rows // tile, score_tile, 0)

    chunk(z)

    height = down_ref.shape[0]
    padded = turned.shape[1]
    batch = layer.shape[0]

    def turn():
        layer_in.wait()
        for d in range(batch):
            piece = layer[d].T
            for c in range(n_ctx):
                rows_c = piece[c * height : (c + 1) * height]
                if padded > height:
                    rows_c = jnp.concatenate(
                        [rows_c.astype(wide), jnp.zeros((padded - height, tokens), wide)], axis=0
                    ).astype(low)
                turned[c, :, d * tokens : (d + 1) * tokens] = rows_c

    value_pairs, value_sends = [], []

    def pair_values():
        others = pl.ds(1, n_dp - 1)
        remote(val_parts.at[others], val_landed.at[others], val_send.at[0], val_recv.at[0], partner).wait_recv()
        total = val_parts[dp].astype(wide)
        for k in range(1, n_dp):
            total = total + val_landed[k].astype(wide)
        piece = val_total.shape[1]
        for c in range(n_ctx):
            val_total[c] = total[c * piece : (c + 1) * piece]
        for k in range(n_z):
            dest = lax.rem(z + k, n_z)
            val_term[k] = val_total[dest * 2 + other].astype(low)
            copy = remote(val_term.at[k], val_pair.at[k], vp_send.at[0], vp_recv.at[0], partner)
            copy.start()
            value_pairs.append(copy)

    def start_values():
        remote(val_term, val_pair, vp_send.at[0], vp_recv.at[0], partner).wait_recv()
        for k in list(range(1, n_z)) + [0]:
            dest = lax.rem(z + k, n_z)
            added = val_total[dest * 2 + core] + val_pair[k].astype(wide)
            if k == 0:
                uv_ref[...] = added
            else:
                val_sum[k] = added.astype(low)
                copy = remote(val_sum.at[k], val_in.at[k], vz_send.at[0], vz_recv.at[0], chip_peer(dest))
                copy.start()
                value_sends.append(copy)

    for at in range(n_z - 1):
        owner = pick(z, line.column(line.arrive, at))
        relay_ok = flag(z, [line.forwards(c, line.arrive[c][at]) for c in range(n_z)])
        copies = []
        if relay_ok is not False:
            end = jnp.where(z == 1, 0, n_z - 1)
            copies = key_copies(owner, relay_send, key_recv, apart(owner), chip_peer(end))
        for n, copy in enumerate(key_copies(owner, key_send, key_recv, apart(owner), partner)):
            copy.wait_recv()
            if copies:
                when(relay_ok, copies[n].start)
        pass_on(owner)
        chunk(owner)
        if at == max(n_z - 3, 0):
            turn()

    top = tops[0]
    for c in range(1, n_z):
        top = jnp.maximum(top, tops[c])
    total = jnp.zeros_like(top)
    for c in range(n_z):
        weight_c = jnp.exp2(tops[c] - top)
        factor[c] = weight_c
        total = total + sums[c] * weight_c
    inverse = 1.0 / total
    for c in range(n_z):
        factor[c] = factor[c] * inverse

    lag, slots = 2, 4
    neighbour = jnp.where(z == 0, 1, n_z - 2)
    at_end = flag(z, [line.hybrid and c in (0, n_z - 1) for c in range(n_z)])

    class Reduce:
        def __init__(self, spans, own, term, landing, total, inbox, relay, acc, sems):
            self.spans = spans
            self.own, self.term, self.landing, self.total = own, term, landing, total
            self.inbox, self.relayed, self.acc = inbox, relay, acc
            self.pair_send, self.pair_recv, self.send, self.recv, self.relay_recv = sems

        def dest(self, at):
            return pick(z, line.column(line.reduce, at))

        def pair(self, at, span, sem):
            return remote(
                self.term.at[at, span], self.landing.at[at, span], self.pair_send.at[0], self.pair_recv.at[sem], partner
            )

        def straight(self, p, at):
            return remote(
                self.total.at[at, self.spans[p]], self.inbox.at[z, self.spans[p]],
                self.send.at[0], self.recv.at[p], chip_peer(self.dest(at)),
            )

        def aside(self, p, at):
            return remote(
                self.total.at[at, self.spans[p]], self.relayed.at[self.spans[p]],
                self.send.at[0], self.relay_recv.at[p], chip_peer(neighbour),
            )

        def consumer(self, at):
            return flag(z, [line.consumes(c, line.reduce[c][at]) for c in range(n_z)])

        def both(self, at, span):
            return self.own[at % slots, span] + self.landing[at, span].astype(wide)

        def begin(self, at, span, sem):
            self.pair(at, span, sem).start()

        def finish(self, at, span, sem):
            self.pair(at, span, sem).wait_recv()
            if at == n_z - 1:
                self.acc[span] = self.both(at, span)
            else:
                self.total[at, span] = self.both(at, span).astype(low)

        def push(self, p, at):
            if at == n_z - 1:
                return
            origin = flag(z, [line.ends(c, line.reduce[c][at]) for c in range(n_z)])

            def out():
                if origin is not False:
                    when(origin, self.aside(p, at).start)
                otherwise(origin, self.straight(p, at).start)

            otherwise(self.consumer(at), out)

        def relay(self, p):
            span = self.spans[p]
            for at in range(n_z - 1):

                def out():
                    self.aside(p, at).wait_recv()
                    self.total[at, span] = (self.both(at, span) + self.relayed[span].astype(wide)).astype(low)
                    self.straight(p, at).start()

                when(self.consumer(at), out)

        def collect(self, p):
            span = self.spans[p]

            def arrived(count):
                blocks = pl.ds(0, count)
                remote(
                    self.total.at[blocks, span], self.inbox.at[blocks, span],
                    self.send.at[0], self.recv.at[p], partner,
                ).wait_recv()

            when(at_end, functools.partial(arrived, n_z - 2))
            otherwise(at_end, functools.partial(arrived, n_z - 1))
            for at in range(n_z - 1):
                source = pick(z, line.column(line.near, at))
                ok = flag(z, [not line.ends(c, line.near[c][at]) for c in range(n_z)])

                def add():
                    self.acc[span] += self.inbox[source, span].astype(wide)

                when(ok, add)

        def sent(self):
            blocks = pl.ds(0, n_z - 1)
            remote(self.term, self.landing, self.pair_send.at[0], self.pair_recv.at[0], partner).wait_send()
            remote(
                self.total.at[blocks], self.inbox.at[blocks], self.send.at[0], self.recv.at[0], partner
            ).wait_send()

    def spans_of(size, tail):
        return [pl.ds(p * size, size + (tail if p == pieces - 1 else 0)) for p in range(pieces)]

    key_fill = pieces * tokens + rope_width
    key_all = pl.ds(0, key_fill)
    key_set = Reduce(
        spans_of(tokens, rope_width), own_k, term_k, landing_k, sum_k, in_k, relay_k, acc_k,
        (kp_send, kp_recv, kz_send, kz_recv, kr_recv),
    )

    def key_terms(at):
        dest = key_set.dest(at)
        keys = pl.ds(pl.multiple_of(dest * chip_rows, chip_rows), chip_rows)
        scale = factor[dest]
        expo[keys, :] = (expo[keys, :].astype(wide) * scale).astype(low)
        slope[keys, :] = (slope[keys, :].astype(wide) * (scale * softmax_scale)).astype(low)
        value = dot(expo[keys, :], grad[...], 1, 0) + dot(slope[keys, :], ql[...], 1, 0)
        rope = dot(qr2t[...], slope[keys, :], 1, 1)
        rope = rope[:rope_width] + rope[rope_width:]
        for c in range(2):
            for p in range(pieces):
                key_stage[c, p * tokens : (p + 1) * tokens, :] = value[
                    c * tokens : (c + 1) * tokens, p * lanes : (p + 1) * lanes
                ]
            key_stage[c, pieces * tokens :, :] = rope[:, c * tokens : (c + 1) * tokens]
        own_k[at % slots] = key_stage[core]
        term_k[at] = key_stage[other].astype(low)

    def key_steps():
        for at in range(n_z + lag):
            if at < n_z:
                key_terms(at)
                key_set.begin(at, key_all, at)
            if at >= lag:
                key_set.finish(at - lag, key_all, at - lag)
                key_set.push(0, at - lag)

    def push_keys(p):
        for at in range(n_z - 1):
            key_set.push(p, at)

    def query_tile(i, carry):
        span = pl.ds(pl.multiple_of(i * tile, tile), tile)
        piece = slope[:, span]
        all_lat = lat_all[...].reshape(n_ctx * tokens, latent)
        dql_ref[span, :] = dot(piece, all_lat, 0, 0).astype(low)
        qrf[span, :] = dot(piece, kr2[...], 0, 0)
        return carry

    def query_terms(step):
        count = rows // tile
        middle = count // 2
        lax.fori_loop(0 if step == 0 else middle, middle if step == 0 else count, query_tile, 0)
        if step == 0:
            return
        for at in range(heads // 2):
            even = qrf[pl.ds(2 * at, tokens, stride=heads), :]
            odd = qrf[pl.ds(2 * at + 1, tokens, stride=heads), :]
            piece = jnp.where(lower, even, odd).T.astype(low)
            dqr_ref[2 * at] = piece[:rope_width]
            dqr_ref[2 * at + 1] = piece[rope_width:]

    def spread_keys(p):
        span = key_set.spans[p]
        message[span] = acc_k[span].astype(low)
        landed[dp, span] = message[span]
        for k in range(1, n_dp):
            remote(
                message.at[span], landed.at[dp, span], dp_send.at[0], dp_recv.at[p], dp_peer(k)
            ).start()
        dlat_ref[:, p * lanes : (p + 1) * lanes] = message[p * tokens : (p + 1) * tokens]
        if p == pieces - 1:
            drope_ref[...] = message[pieces * tokens :]

    packed = height % 32 == 0
    rope_rows = height // 2 if packed else padded
    down_set = Reduce(
        spans_of(padded, rope_rows), own_d, term_d, pair_d, sum_d, in_d, relay_d, acc_d,
        (gp_send, gp_recv, gz_send, gz_recv, gr_recv),
    )

    def down_piece(p, index):
        every = landed[:, p * tokens : (p + 1) * tokens, :].reshape(batch * tokens, lanes)
        lat = dot(turned[index], every, 1, 0)
        if p < pieces - 1:
            return lat
        if packed:
            rope = dot(turned[index, : height // 2], rope_lo[...], 1, 1)
            rope = rope + dot(turned[index, height // 2 :], rope_hi[...], 1, 1)
        else:
            rope = dot(turned[index], rope_lo[...], 1, 1)
        return jnp.concatenate([lat, rope], axis=0)

    def down_terms(p):
        others = pl.ds(0, n_dp - 1)
        arrived = landed.at[others, key_set.spans[p]]
        remote(arrived, arrived, dp_send.at[0], dp_recv.at[p], partner).wait_recv()
        if p == pieces - 1:
            for b in range(batch):
                piece = landed[b, pieces * tokens :, :]
                cols = slice(b * tokens, (b + 1) * tokens)
                rope_lo[:rope_width, cols] = piece
                rope_hi[rope_width:, cols] = piece
            rope_lo[rope_width:, :] = jnp.zeros((rope_width, batch * tokens), low)
            rope_hi[:rope_width, :] = jnp.zeros((rope_width, batch * tokens), low)
        span = down_set.spans[p]
        for at in range(n_z + lag):
            if at < n_z:
                dest = down_set.dest(at)
                term_d[at, span] = down_piece(p, dest * 2 + other).astype(low)
                down_set.begin(at, span, p * n_z + at)
                own_d[at % slots, span] = down_piece(p, dest * 2 + core)
            if at >= lag:
                down_set.finish(at - lag, span, p * n_z + at - lag)
                down_set.push(p, at - lag)

    key_steps()
    push_keys(1)
    key_set.relay(0)
    push_keys(2)
    query_terms(0)
    key_set.relay(1)
    push_keys(3)
    key_set.collect(0)
    spread_keys(0)
    pair_values()
    key_set.relay(2)
    key_set.collect(1)
    spread_keys(1)
    query_terms(1)
    key_set.relay(3)
    start_values()
    down_terms(0)
    key_set.collect(2)
    spread_keys(2)
    down_terms(1)
    key_set.collect(3)
    spread_keys(3)
    down_set.relay(0)
    down_terms(2)
    down_set.relay(1)
    down_terms(3)
    down_set.relay(2)
    down_set.relay(3)
    others = pl.ds(1, n_z - 1)
    remote(val_sum.at[others], val_in.at[others], vz_send.at[0], vz_recv.at[0], partner).wait_recv()
    for k in range(1, n_z):
        uv_ref[...] += val_in[k].astype(wide)
    for p in range(pieces):
        down_set.collect(p)
        down_ref[:, p * lanes : (p + 1) * lanes] = acc_d[p * padded : p * padded + height]
    rope = acc_d[pieces * padded :]
    if packed:
        down_ref[: height // 2, latent:] = rope[:, :rope_width]
        down_ref[height // 2 :, latent:] = rope[:, rope_width:]
    else:
        down_ref[:, latent:] = rope[:height, :rope_width]

    when(at_end, functools.partial(key_blocks_sent, key_send, n_z - 2))
    otherwise(at_end, functools.partial(key_blocks_sent, key_send, n_z - 1))
    key_blocks_sent(fwd_send, n_z)
    relays = flag(z, [line.hybrid and c in (1, n_z - 2) for c in range(n_z)])
    when(relays, functools.partial(key_blocks_sent, relay_send, 1))
    others = pl.ds(0, n_dp - 1)
    remote(val_parts.at[others], val_landed.at[others], val_send.at[0], val_recv.at[0], partner).wait_send()
    remote(val_term, val_pair, vp_send.at[0], vp_recv.at[0], partner).wait_send()
    others = pl.ds(0, n_z - 1)
    remote(val_sum.at[others], val_in.at[others], vz_send.at[0], vz_recv.at[0], partner).wait_send()
    key_set.sent()
    down_set.sent()
    sent = landed.at[pl.ds(0, n_dp - 1)]
    remote(sent, sent, dp_send.at[0], dp_recv.at[0], partner).wait_send()


def store_kernel(n, *refs):
    sem = refs[2 * n]
    copies = []
    for at in range(n):
        rows = refs[at].shape[0]
        parts = 4 if rows % 64 == 0 and rows >= 512 else 1
        for part in range(parts):
            span = pl.ds(part * (rows // parts), rows // parts)
            copies.append(pltpu.make_async_copy(refs[at].at[span], refs[n + at].at[span], sem.at[len(copies)]))
    for copy in copies:
        copy.start()
    for copy in copies:
        copy.wait()


def body(n_dp, n_ctx, layer_input, kv_latent, key_rope, q_latent, q_rope, saved_output, w_uv, d_out, blocks):
    tokens = kv_latent.shape[1]
    heads, latent = q_latent.shape[2], q_latent.shape[3]
    rope_width = key_rope.shape[2]
    rows = tokens * heads
    seq_rows = tokens * n_ctx
    n_z = n_ctx // 2
    values = w_uv.shape[1]
    batch, _, width = layer_input.shape
    height = width // n_ctx
    padded = -(-height // 16) * 16
    down_fill = 4 * padded + (height // 2 if height % 32 == 0 else padded)
    key_fill = 4 * tokens + rope_width
    pieces = 4
    share = latent // (n_dp * n_ctx)
    two = 2 * rope_width
    vmem = pl.BlockSpec(memory_space=pltpu.VMEM)
    hbm = pl.BlockSpec(memory_space=pltpu.HBM)
    dma = lambda n: pltpu.SemaphoreType.DMA((n,))

    def stage(fill):
        half = lambda *dims: pltpu.VMEM((*dims, fill, 128), low)
        return [
            pltpu.VMEM((4, fill, 128), wide), half(n_z), half(n_z), half(n_z), half(n_z), half(),
            pltpu.VMEM((fill, 128), wide),
        ]

    outs = (
        ((rows, latent), low),
        ((heads, rope_width, tokens), low),
        ((tokens, latent), low),
        ((rope_width, tokens), low),
        ((height, latent + rope_width), wide),
        ((share, values), wide),
    )
    found = pl.pallas_call(
        functools.partial(main_kernel, n_dp, n_ctx),
        out_shape=tuple(pltpu.VMEM(shape, kind) for shape, kind in outs),
        in_specs=[pl.BlockSpec(memory_space=pltpu.SMEM)] + [hbm] * 8,
        out_specs=(vmem,) * 6,
        scratch_shapes=[
            pltpu.VMEM((n_ctx, tokens, latent), low),
            pltpu.VMEM((n_ctx, rope_width, tokens), low),
            pltpu.VMEM((seq_rows, two), low),
            pltpu.VMEM((rows, latent), low),
            pltpu.VMEM((heads, rope_width, tokens), low),
            pltpu.VMEM((rows, two), wide),
            pltpu.VMEM((rows, two), low),
            pltpu.VMEM((two, rows), low),
            pltpu.VMEM((rows, latent), low),
            pltpu.VMEM((latent, values), low),
            pltpu.VMEM((tokens, values), low),
            pltpu.VMEM(layer_input.shape, low),
            pltpu.VMEM((n_ctx, padded, batch * tokens), low),
            pltpu.VMEM((rows, values), low),
            pltpu.VMEM((rows, latent), low),
            pltpu.VMEM((1, rows), wide),
            pltpu.VMEM((seq_rows, 1), jnp.int32),
            pltpu.VMEM((seq_rows, rows), low),
            pltpu.VMEM((seq_rows, rows), low),
            pltpu.VMEM((n_z, 1, rows), wide),
            pltpu.VMEM((n_z, 1, rows), wide),
            pltpu.VMEM((n_z, 1, rows), wide),
            pltpu.VMEM((n_dp, latent // n_dp, values), low),
            pltpu.VMEM((n_dp, latent // n_dp, values), low),
            pltpu.VMEM((n_ctx, share, values), wide),
            pltpu.VMEM((n_z, share, values), low),
            pltpu.VMEM((n_z, share, values), low),
            pltpu.VMEM((n_z, share, values), low),
            pltpu.VMEM((n_z, share, values), low),
            pltpu.VMEM((2, key_fill, 128), wide),
            *stage(key_fill),
            pltpu.VMEM((key_fill, 128), low),
            pltpu.VMEM((n_dp, key_fill, 128), low),
            *stage(down_fill),
            pltpu.VMEM((two, batch * tokens), low),
            pltpu.VMEM((two, batch * tokens), low),
            dma(8), dma(2), dma(3 * n_z), dma(2), dma(n_z), dma(2),
            dma(1), dma(1), dma(1), dma(1), dma(1), dma(1),
            dma(1), dma(n_z), dma(1), dma(pieces), dma(pieces),
            dma(1), dma(pieces * n_z), dma(1), dma(pieces), dma(pieces),
            dma(1), dma(pieces),
        ],
        compiler_params=pltpu.CompilerParams(
            collective_id=0, has_side_effects=True, vmem_limit_bytes=VMEM_LIMIT
        ),
        name="main",
    )(
        blocks, kv_latent[0], key_rope[0].T,
        q_latent[0].reshape(rows, latent), jnp.transpose(q_rope[0], (1, 2, 0)),
        saved_output[0].reshape(rows, latent), w_uv, d_out[0], layer_input,
    )
    d_lat, d_rope, k_lat, k_rope, grad_down, grad_uv = pl.pallas_call(
        functools.partial(store_kernel, len(outs)),
        out_shape=tuple(jax.ShapeDtypeStruct(shape, kind) for shape, kind in outs),
        in_specs=[vmem] * len(outs),
        out_specs=(hbm,) * len(outs),
        scratch_shapes=[dma(len(outs) + 3)],
        compiler_params=pltpu.CompilerParams(vmem_limit_bytes=4 * 1024 * 1024),
        name="store",
    )(*found)
    return (
        d_lat.reshape(1, tokens, heads, latent),
        jnp.transpose(d_rope, (2, 0, 1))[None],
        k_lat[None],
        k_rope.T[None],
        grad_down,
        grad_uv,
    )


def solution(mesh):
    n_dp, n_ctx = mesh.shape["dp"], mesh.shape["ctx"]
    in_specs = (
        P(None, "ctx", "dp"),
        P("dp", "ctx", None),
        P("dp", "ctx", None),
        P("dp", "ctx", None, None),
        P("dp", "ctx", None, None),
        P("dp", "ctx", None, None),
        P(),
        P("dp", "ctx", None),
        P(),
    )
    out_specs = (
        P("dp", "ctx", None, None),
        P("dp", "ctx", None, None),
        P("dp", "ctx", None),
        P("dp", "ctx", None),
        P(("dp", "ctx"), None),
        P(("dp", "ctx"), None),
    )
    return jax.shard_map(
        functools.partial(body, n_dp, n_ctx),
        mesh=mesh, in_specs=in_specs, out_specs=out_specs, check_vma=False,
    )
```
